32 devices in a mesh: band: 16 (over z, y, core), spin: 2 (over x).
Axes of the slice: x: 2, y: 2, z: 4, core: 2. Of those that a mesh axis runs over, the one named last changes fastest.
Arguments:
- coefficients: bfloat16 [2, 2, 32, 524288], P('spin', None, 'band'), may hold values from -1 to 1
- occupation: int32 [2, 32], P('spin', 'band'), may hold values from 0 to 1000
- miller: int32 [3, 524288], P(None, ('band', 'spin')), may hold values from -8 to 8
- density: float32 [2, 256, 128, 128], P('spin', 'band'), may hold values from 0.25 to 2
- local_factor: float32 [2, 256, 128, 128], P(None, None, 'band'), may hold values from -1.2 to 1.2
Outputs:
- stress: float32 [6], replicated
- kinetic_density: float32 [524288], P(('band', 'spin'))
- gradient_square: float32 [2, 256, 128, 128], P('spin', 'band')
The draws below stay inside these ranges and needn't reach their ends.
All inputs are finite; a program needn't handle non-finite values.
Results may differ from the reference program's by a relative error of at most 0.0003.
Values sent between devices are 32-bit elements; how exact they have to be, the bound alone decides.
A program may use at most 64 MiB of HBM per device.

```python
import math
import jax
import jax.numpy as jnp
from jax import lax

NPW = 524288
NX = 128
NY = 128
NZ = 256
BANDS = 32
SPINS = 2


def place_ends(result, stream_key, smallest, high):
    longest = result.shape.index(max(result.shape))
    spots = []
    for shift in (0, 1):
        where = [jax.random.randint(jax.random.fold_in(stream_key, axis), (), 0, length) for axis, length in enumerate(result.shape)]
        where[longest] = (where[longest] + shift) % result.shape[longest]
        spots.append(tuple(where))
    return result.at[spots[0]].set(smallest).at[spots[1]].set(high)


def with_spikes(values, rng, source, target, parts, factor):
    def block_of(dim):
        return (jnp.arange(values.shape[dim]) // (values.shape[dim] // parts)).reshape((-1,) + (1,) * (values.ndim - 1 - dim))

    one_side = jax.random.permutation(rng, parts)[block_of(target)]
    other_side = (block_of(target) + parts // 2) % parts
    return jnp.where((block_of(source) == one_side) | (block_of(source) == other_side), factor * values, values)


def steps_of(rng, dims, split, low, largest):
    def one(axis_at, blocks):
        draws = jax.random.uniform(jax.random.fold_in(jax.random.fold_in(rng, 6), axis_at), (blocks,), jnp.float32, low / len(split), largest / len(split))
        return jnp.repeat(jnp.exp(draws), dims[axis_at] // blocks).reshape((-1,) + (1,) * (len(dims) - axis_at - 1))

    level = one(*split[0])
    for cut in split[1:]:
        level = level * one(*cut)
    return level


def bell_draw(rng, dims, deviation, reach, split=(), kind=jnp.bfloat16):
    loudness = steps_of(rng, dims, split, -0.22, 0.18) if split else 1.0
    values = jax.random.normal(rng, dims, jnp.float32) * deviation * loudness
    return jnp.minimum(jnp.maximum(values, -reach), reach).astype(kind)


def heavy_noise(key, shape, width, limit, split, heavy, held_as=jnp.bfloat16):
    entries = width * jax.random.normal(key, shape, jnp.float32)
    if split:
        entries = entries * steps_of(key, shape, split, -0.22, 0.18)
    return jnp.clip(with_spikes(entries, jax.random.fold_in(key, 3), *heavy), -limit, limit).astype(held_as)


def setup_inputs(seed: int = 0) -> dict:
    keys = jax.random.split(jax.random.key(seed), 6)
    coefficients = heavy_noise(keys[0], (SPINS, 2, BANDS, NPW), (2 * BANDS) ** -0.5, 1.0, ((0, 2), (2, 16)), (2, 3, 16, 2.0))
    occupation = place_ends(jax.random.randint(keys[1], (SPINS, BANDS), 0, 1001), jax.random.fold_in(keys[1], 1), 0, 1000).astype(jnp.int32)
    miller = place_ends(jax.random.randint(keys[2], (3, NPW), -8, 9), jax.random.fold_in(keys[2], 1), -8, 8).astype(jnp.int32)
    density = jnp.clip(0.25 + 1.75 * jax.random.uniform(keys[3], (SPINS, NZ, NX, NY), jnp.float32) ** steps_of(keys[3], (SPINS, NZ, NX, NY), ((0, 2), (1, 16)), -0.2, 0.2), 0.25, 2.0)
    local_factor = bell_draw(keys[4], (2, NZ, NX, NY), 0.2, 1.2, ((2, 16),), jnp.float32)
    return {"coefficients": coefficients, "occupation": occupation, "miller": miller, "density": density, "local_factor": local_factor}


occupation_unit = 1000.0
kpoint = (0.25, 0.125, 0.375)
spacing = 0.25


def derivative_table(length):
    row_index = jnp.arange(length, dtype=jnp.int32)[:, None]
    col_index = jnp.arange(length, dtype=jnp.int32)[None, :]
    wrapped = jnp.mod(row_index - col_index, length)
    angles = (jnp.pi / length) * wrapped.astype(jnp.float32)
    on_diagonal = wrapped == 0
    sines = jnp.where(on_diagonal, 1.0, jnp.sin(angles))
    parity = 1.0 - 2.0 * jnp.mod(wrapped, 2).astype(jnp.float32)
    return jnp.where(on_diagonal, 0.0, 0.5 * parity * jnp.cos(angles) / sines).astype(jnp.float32)


def frequencies(length):
    positions = jnp.arange(length, dtype=jnp.int32)
    signed = jnp.where(positions >= length // 2, positions - length, positions)
    return (2.0 * jnp.pi / length) * signed.astype(jnp.float32)


def six_sums(weighting, first_axis, second_axis, third_axis):
    return jnp.stack([
        jnp.sum(weighting * first_axis * first_axis),
        jnp.sum(weighting * second_axis * second_axis),
        jnp.sum(weighting * third_axis * third_axis),
        jnp.sum(weighting * second_axis * third_axis),
        jnp.sum(weighting * first_axis * third_axis),
        jnp.sum(weighting * first_axis * second_axis)])


def reference(coefficients, occupation, miller, density, local_factor):
    highest = lax.Precision.HIGHEST
    weights = occupation.astype(jnp.float32) / occupation_unit
    band_block = math.gcd(BANDS, 32)

    def accumulate(counter, running):
        first_row = (jnp.asarray(counter).astype(jnp.int32) * band_block).astype(jnp.int32)
        piece = lax.dynamic_slice_in_dim(coefficients, first_row, band_block, 2).astype(jnp.float32)
        squares = piece[:, 0] * piece[:, 0] + piece[:, 1] * piece[:, 1]
        weight_piece = lax.dynamic_slice_in_dim(weights, first_row, band_block, 1)
        return running + jnp.einsum('sb,sbg->g', weight_piece, squares, precision=highest)

    kinetic_weight = lax.fori_loop(0, BANDS // band_block, accumulate, jnp.zeros((NPW,), jnp.float32))
    kvec = jnp.array(kpoint, jnp.float32)
    gvec = spacing * (miller.astype(jnp.float32) + kvec[:, None])
    kinetic_density = 0.5 * (gvec[0] ** 2 + gvec[1] ** 2 + gvec[2] ** 2) * kinetic_weight
    kinetic_stress = -six_sums(kinetic_weight, gvec[0], gvec[1], gvec[2]) / NPW

    deriv_x = derivative_table(NX)
    deriv_y = derivative_table(NY)
    deriv_z = derivative_table(NZ)
    grad_x = jnp.einsum('ik,szky->sziy', deriv_x, density, precision=highest)
    grad_y = jnp.einsum('ik,szxk->szxi', deriv_y, density, precision=highest)
    grad_z = jnp.einsum('ik,skxy->sixy', deriv_z, density, precision=highest)
    gradient_square = grad_x * grad_x + grad_y * grad_y + grad_z * grad_z
    kernel = density ** (-1.0 / 3.0) / (1.0 + gradient_square / (4.0 * density * density + 1.0))
    cell_count = NZ * NX * NY
    xc_stress = -six_sums(kernel, grad_x, grad_y, grad_z) / cell_count

    total_density = jnp.sum(density, axis=0)
    spectrum = jnp.fft.fftn(total_density) / cell_count
    real_part = jnp.real(spectrum)
    imag_part = jnp.imag(spectrum)
    freq_z = frequencies(NZ)[:, None, None]
    freq_x = frequencies(NX)[None, :, None]
    freq_y = frequencies(NY)[None, None, :]
    length_sq = freq_x * freq_x + freq_y * freq_y + freq_z * freq_z
    positive = length_sq > 0
    inverse = jnp.where(positive, 1.0 / jnp.where(positive, length_sq, 1.0), 0.0)
    hartree_weight = 4.0 * jnp.pi * (real_part * real_part + imag_part * imag_part) * inverse
    diagonal = jnp.array([1.0, 1.0, 1.0, 0.0, 0.0, 0.0], jnp.float32)
    hartree_stress = 2.0 * six_sums(hartree_weight * inverse, freq_x, freq_y, freq_z) - diagonal * jnp.sum(hartree_weight)
    local_weight = 2.0 * (real_part * local_factor[0] + imag_part * local_factor[1])
    local_stress = six_sums(local_weight, freq_x, freq_y, freq_z)
    stress = kinetic_stress + hartree_stress + local_stress + xc_stress
    return stress, kinetic_density, gradient_square
```

```python
import functools

import jax
import jax.numpy as jnp
import numpy as np
from jax import lax
from jax.experimental import pallas as pl
from jax.experimental.pallas import tpu as pltpu
from jax.sharding import PartitionSpec as P

occupation_unit = 1000.0
kpoint = (0.25, 0.125, 0.375)
spacing = 0.25
MESH = pl.DeviceIdType.MESH
VMEM = pl.BlockSpec(memory_space=pltpu.VMEM)
CHUNKS = 2


def derivative_table(length):
    index = np.arange(length)
    wrapped = np.mod(index[:, None] - index[None, :], length)
    angles = np.pi / length * wrapped
    sines = np.where(wrapped == 0, 1.0, np.sin(angles))
    parity = 1.0 - 2.0 * np.mod(wrapped, 2)
    table = np.where(wrapped == 0, 0.0, 0.5 * parity * np.cos(angles) / sines)
    return table.astype(np.float32)


def fourier_tables(length):
    index = np.arange(length)
    phases = np.mod(index[:, None] * index[None, :], length) * (2.0 * np.pi / length)
    return np.cos(phases), np.sin(phases)


def greet_all(nb, ns):
    b, s = lax.axis_index("band"), lax.axis_index("spin")
    barrier = pltpu.get_barrier_semaphore()

    def greet(k, carry):
        pl.semaphore_signal(
            barrier,
            inc=1,
            device_id=((b + k // ns) % nb, (s + k % ns) % ns),
            device_id_type=MESH,
        )
        return carry

    lax.fori_loop(1, nb * ns, greet, 0)
    pl.semaphore_wait(barrier, nb * ns - 1)
    return b, s


def far_first(k, count):
    return 1 + (k + count // 2 - 1) % (count - 1)


def split(value):
    high = value.astype(jnp.bfloat16)
    return high, (value - high.astype(jnp.float32)).astype(jnp.bfloat16)


def host_split(table):
    high = table.astype(np.float32).astype(jnp.bfloat16)
    low = (table - high.astype(np.float64)).astype(np.float32).astype(jnp.bfloat16)
    return np.stack([high, low])


def dot3(left, right):
    def one(p, q):
        return jnp.dot(p, q, preferred_element_type=jnp.float32)

    return one(left[0], right[0]) + (one(left[0], right[1]) + one(left[1], right[0]))


def loop(low, high, step):
    def body(k, carry):
        step(k)
        return carry

    lax.fori_loop(low, high, body, 0)


def axis_frequency(index, length):
    signed = jnp.where(index >= length // 2, index - length, index)
    return 2.0 * np.pi / length * signed.astype(jnp.float32)


def fold(value):
    return jnp.sum(value, axis=0, keepdims=True)


def guard(always, condition, step):
    if always:
        step()
    else:
        pl.when(condition)(step)


def stack3(left, right):
    high, low = right
    depth = high.shape[0]
    return jnp.dot(
        left, jnp.concatenate([high, high], axis=0), preferred_element_type=jnp.float32
    ) + jnp.dot(left[:, :depth], low, preferred_element_type=jnp.float32)


def main_kernel(
    nb, ns, ny, nz, occupation, dens_h, coef_h, factor_h,
    table_f_h, table_i_h, table_y_h, table_d_h, table_z_h, table_g_h, pairs_h, miller_h,
    stress, kdens, square,
    dens, coef, factor, table_f, table_i, table_y, table_d, table_z, table_g, pairs, miller,
    kin, out, col, grad, gout, from_core, sum_core, from_plane, sum_plane, from_line,
    inverses, grad_x, grad_y, part, row, held,
    f_sem, d_send, d_recv, c_send, c_recv, p_send, p_recv, l_send, l_recv,
    g_send, g_recv, t_send, t_recv,
):
    sources = (dens_h, table_f_h, coef_h, pairs_h, table_g_h, table_d_h, table_y_h, table_z_h, factor_h, table_i_h, miller_h)
    targets = (dens, table_f, coef, pairs, table_g, table_d, table_y, table_z, factor, table_i, miller)
    fetches = [
        pltpu.make_async_copy(source, target, f_sem.at[i])
        for i, (source, target) in enumerate(zip(sources, targets))
    ]
    for fetch in fetches:
        fetch.start()
    b, s = greet_all(nb, ns)
    n = nb * ns
    core, y, z = b % 2, (b // 2) % ny, b // (2 * ny)
    zl, nx, width = dens.shape
    chunks, _, _, block, _ = col.shape
    hb = nb // 2
    half, u = b // hb, b % hb
    xl = nx // nb
    na = min(ns, xl)
    per = xl // na
    each = per // chunks
    rc = 2 * each
    zp = block // rc
    hz = hb * zl
    nzg = nb * zl
    rows = kdens.shape[0]
    whole, mine = na == ns, s < na
    for fetch in fetches[:2]:
        fetch.wait()

    def peer(k, count):
        offset = far_first(k, count * ns)
        return (offset // ns, (s + offset % ns) % ns)

    def block_copy(c, k):
        step, ts = peer(k, nb)
        tb = (b + step) % nb
        at = pl.multiple_of((tb * na + ts) * block, block)
        return ts < na, pltpu.make_async_remote_copy(
            out.at[c, pl.ds(at, block), :], col.at[c, s, b], d_send.at[c, k], d_recv.at[c, k],
            device_id=(tb, ts), device_id_type=MESH,
        )

    for c in range(chunks):

        def forward(i):
            value = split(jnp.concatenate([dens[2 * i], dens[2 * i + 1]], axis=1))
            turned = stack3(table_f[c], value)
            out[c, pl.ds(2 * i, nb * na * rc, stride=zp), :] = turned[:, :width]
            out[c, pl.ds(2 * i + 1, nb * na * rc, stride=zp), :] = turned[:, width:]

        loop(0, zl // 2, forward)

        def send(k):
            right, copy = block_copy(c, k)
            guard(whole, right, copy.start)

        loop(0, n - 1, send)

        def keep():
            at = pl.multiple_of((b * na + s) * block, block)
            col[c, s, b] = out[c, pl.ds(at, block), :]

        guard(whole, mine, keep)

    nbl = occupation.shape[1]
    depth = rows * nbl
    band = lax.broadcasted_iota(jnp.int32, (depth, 128), 0) % nbl
    weight = jnp.zeros((depth, 128), jnp.float32)
    for j in range(nbl):
        share = jnp.full((depth, 128), occupation[0, j]).astype(jnp.float32) / occupation_unit
        weight = jnp.where(band == j, share, weight)
    for fetch in fetches[2:4]:
        fetch.wait()

    def kinetic(i):
        here = pl.ds(pl.multiple_of(i * depth, depth), depth)
        real, imag = coef[0, here, :].astype(jnp.float32), coef[1, here, :].astype(jnp.float32)
        high, low = split(weight * (real * real + imag * imag))
        kin[i // (2 * ns), (i // ns) % 2, i % ns] = jnp.dot(
            pairs[...], high, preferred_element_type=jnp.float32
        ) + jnp.dot(pairs[...], low, preferred_element_type=jnp.float32)

    loop(0, n, kinetic)
    core_copy = pltpu.make_async_remote_copy(
        kin.at[:, 1 - core], from_core, c_send.at[0], c_recv.at[0],
        device_id=(b + 1 - 2 * core, s), device_id_type=MESH,
    )
    core_copy.start()

    fetches[4].wait()

    def in_plane(i):
        value = split(dens[i])
        grad_x[i] = dot3((table_g[0, 0], table_g[1, 0]), value)
        grad_y[i] = dot3(value, (table_g[0, 1], table_g[1, 1]))

    loop(0, zl, in_plane)

    core_copy.wait()

    def add_core(i):
        sum_core[i // ny, i % ny] = kin[i, core] + from_core[i]

    loop(0, nz * ny, add_core)
    plane_copies = []
    for k in range(1, ny * ns):
        ty, ts = (y + k // ns) % ny, (s + k % ns) % ns
        copy = pltpu.make_async_remote_copy(
            sum_core.at[:, ty, ts], from_plane.at[k - 1], p_send.at[k - 1], p_recv.at[k - 1],
            device_id=((z * ny + ty) * 2 + core, ts), device_id_type=MESH,
        )
        copy.start()
        plane_copies.append(copy)

    freq_z = axis_frequency(lax.broadcasted_iota(jnp.int32, (nzg, width), 0), nzg)
    freq_y = axis_frequency(lax.broadcasted_iota(jnp.int32, (nzg, width), 1), width)
    row_y = freq_y[:1]

    def place(j):
        return b * xl + s * per + j

    def invert(j):
        freq_x = axis_frequency(jnp.full((nzg, width), place(j)), nx)
        length = freq_x * freq_x + freq_y * freq_y + freq_z * freq_z
        positive = length > 0
        inverses[j] = jnp.where(positive, 1.0 / jnp.where(positive, length, 1.0), 0.0)

    loop(0, per, invert)

    for copy in plane_copies:
        copy.wait()
    total = sum_core[:, y, s]
    for k in range(1, ny * ns):
        total = total + from_plane[k - 1]
    sum_plane[...] = total

    def line_copy(k):
        tz = (z + k) % nz
        return pltpu.make_async_remote_copy(
            sum_plane.at[tz], from_line.at[k - 1], l_send.at[k - 1], l_recv.at[k - 1],
            device_id=((tz * ny + y) * 2 + core, s), device_id_type=MESH,
        )

    loop(1, nz, lambda k: line_copy(k).start())
    part[...] = jnp.zeros_like(part)
    for fetch in fetches[5:10]:
        fetch.wait()

    def back_copy(c, k):
        step, ts = peer(k, hb)
        tu = (u + step) % hb
        at = pl.multiple_of(((c * hb + u) * na + s) * block, block)
        return (s - (ts - s)) % ns < na, pltpu.make_async_remote_copy(
            grad.at[c, ts, tu], gout.at[pl.ds(at, block), :], g_send.at[c, k], g_recv.at[c, k],
            device_id=(half * hb + tu, ts), device_id_type=MESH,
        )

    def column(c, k, r):
        return col[c, k, :, pl.ds(pl.multiple_of(r * zp, zp), zl), :].reshape(nzg, width)

    rows_d = pl.ds(pl.multiple_of(half * hz, hz), hz)
    for c in range(chunks):

        def receive(k):
            right, copy = block_copy(c, k)
            guard(whole, right, copy.wait_send)
            guard(whole, mine, copy.wait_recv)

        loop(0, n - 1, receive)

        def derive(j):
            k, r = j // each, 2 * (j % each)
            value = split(jnp.concatenate([column(c, k, r), column(c, k, r + 1)], axis=1))
            slope = dot3((table_d[0, rows_d, :], table_d[1, rows_d, :]), value)
            for i in range(2):
                here = pl.ds(pl.multiple_of((r + i) * zp, zp), zl)
                grad[c, k, :, here, :] = slope[:, i * width:(i + 1) * width].reshape(hb, zl, width)

        def give_back(k):
            back_copy(c, k)[1].start()

        def local_back():
            at = pl.multiple_of(((c * hb + u) * na + s) * block, block)
            gout[pl.ds(at, block), :] = grad[c, s, u]

        def transform(i):
            j = c * each + i
            real, imag = column(c, 0, i), column(c, 0, each + i)
            for k in range(1, ns):
                real, imag = real + column(c, k, i), imag + column(c, k, each + i)
            position = jnp.full((nzg, width), place(j))
            imag = jnp.where(position % (nx // 2) == 0, 0.0, imag)
            value = split(jnp.concatenate([real, imag], axis=1))
            value = split(dot3(value, (table_y[0], table_y[1])))
            turned = dot3((table_z[0], table_z[1]), value)
            real = turned[:nzg, :width] + turned[nzg:, width:]
            imag = turned[:nzg, width:] - turned[nzg:, :width]
            inverse = inverses[j]
            here = s * per + j
            local = real * factor[0, :, here, :] + imag * factor[1, :, here, :]
            hartree = (4.0 * np.pi) * (real * real + imag * imag) * inverse
            weigh = 2.0 * (hartree * inverse + local)
            weigh_z = weigh * freq_z
            plain, along_z, along_zz = fold(weigh), fold(weigh_z), fold(weigh_z * freq_z)
            trace = fold(hartree)
            row_x = axis_frequency(position[:1], nx)
            terms = (
                plain * row_x * row_x - trace,
                plain * row_y * row_y - trace,
                along_zz - trace,
                along_z * row_y,
                along_z * row_x,
                plain * row_x * row_y,
            )
            for i, term in enumerate(terms):
                part[pl.ds(i, 1), :] += term

        def work():
            loop(0, ns * each, derive)
            loop(0, hb * ns - 1, give_back)
            local_back()
            loop(0, each, transform)

        guard(whole, mine, work)

    loop(1, nz, lambda k: line_copy(k).wait())
    kweight = sum_plane[z] + jnp.sum(from_line[...], axis=0)
    fetches[10].wait()
    gk = [spacing * (miller[i].reshape(rows, 128).astype(jnp.float32) + kpoint[i]) for i in range(3)]
    kdens[...] = 0.5 * (gk[0] * gk[0] + gk[1] * gk[1] + gk[2] * gk[2]) * kweight
    scaled = kweight * (-1.0 / (n * rows * 128))
    order = ((0, 0), (1, 1), (2, 2), (1, 2), (0, 2), (0, 1))
    for i, (p, q) in enumerate(order):
        part[pl.ds(i, 1), :] += fold(scaled * gk[p] * gk[q])

    for c in range(chunks):

        def collect(k):
            right, copy = back_copy(c, k)
            guard(whole, mine, copy.wait_send)
            guard(whole, right, copy.wait_recv)

        loop(0, hb * ns - 1, collect)

    def exchange(i):
        slope = jnp.concatenate(
            [gout[pl.ds(2 * i + j, nx, stride=zp), :] for j in range(2)], axis=1
        )
        slope = stack3(table_i[half], split(slope))
        for j in range(2):
            value = dens[2 * i + j]
            g = (grad_x[2 * i + j], grad_y[2 * i + j], slope[:, j * width:(j + 1) * width])
            total = g[0] * g[0] + g[1] * g[1] + g[2] * g[2]
            square[2 * i + j] = total
            scale = 4.0 * value * value + 1.0
            weigh = jnp.exp(jnp.log(value) * (-1.0 / 3.0)) * scale / (scale + total)
            weigh = weigh * (-1.0 / (nzg * nx * width))
            for t, (p, q) in enumerate(order):
                part[pl.ds(t, 1), :] += fold(weigh * g[p] * g[q])

    loop(0, zl // 2, exchange)
    spots = [lax.broadcasted_iota(jnp.int32, (8, 128), i) for i in range(2)]
    sums = jnp.sum(part[...], axis=1, keepdims=True)
    row[...] = fold(jnp.where(spots[0] == spots[1], sums, 0.0))

    def stress_copy(k):
        tb, ts = (b + k // ns) % nb, (s + k % ns) % ns
        return pltpu.make_async_remote_copy(
            row, held.at[k - 1], t_send.at[k - 1], t_recv.at[k - 1],
            device_id=(tb, ts), device_id_type=MESH,
        )

    loop(1, n, lambda k: stress_copy(k).start())
    loop(1, n, lambda k: stress_copy(k).wait())
    stress[...] = row[...] + jnp.sum(held[...], axis=0)


def params(number):
    return pltpu.CompilerParams(
        collective_id=number, has_side_effects=True, vmem_limit_bytes=60 * 2**20
    )


def f32(*shape):
    return jax.ShapeDtypeStruct(shape, jnp.float32)


def real_basis(nb, na, chunks, nx):
    xl = nx // nb
    per = xl // na
    each = per // chunks
    x = np.arange(nx)
    basis = np.zeros((chunks, nb, na, 2, each, nx))
    share = np.zeros((chunks, nb, na, 2, each))
    for b in range(nb):
        for j in range(xl):
            k = b * xl + j
            phases = (2.0 * np.pi / nx) * ((k * x) % nx)
            spot = (j % per // each, b, j // per, slice(None), j % each)
            if k % (nx // 2) == 0:
                other = (2.0 * np.pi / nx) * (((nx // 2 - k) * x) % nx)
                basis[spot] = np.stack([np.cos(phases), np.cos(other)])
                share[spot] = 1.0 / nx
            else:
                basis[spot] = np.stack([np.cos(phases), -np.sin(phases)])
                share[spot] = 2.0 / nx
    inverse = (basis * share[..., None]).reshape(chunks, 2, nb // 2, -1, nx)
    inverse = inverse.transpose(1, 4, 0, 2, 3).reshape(2, nx, nx)
    return basis.reshape(chunks, -1, nx), inverse


def beside(table):
    return np.concatenate(list(host_split(table)), axis=-1)


def shards(nb, ns, coefficients, occupation, miller, density, local_factor):
    dma = pltpu.SemaphoreType.DMA
    _, zl, nx, ny = density.shape
    nzg = zl * nb
    xl = nx // nb
    na = min(ns, xl)
    per = xl // na
    chunks = min(CHUNKS, per)
    rc = 2 * (per // chunks)
    zp = zl
    while rc * zp % 8:
        zp += 1
    block = rc * zp
    npw = coefficients.shape[3]
    rows = npw // (nb * ns * 128)
    nbl = coefficients.shape[2]
    fold_y = 2 if nb % 4 == 0 else 1
    fold_z = nb // (2 * fold_y)
    hb = nb // 2

    coef = coefficients[0].reshape(2, nbl, npw // 128, 128)
    coef = coef.transpose(0, 2, 1, 3).reshape(2, npw // 128 * nbl, 128)
    pairs = jnp.asarray(np.kron(np.eye(rows), np.ones((1, nbl))), jnp.bfloat16)
    basis, inverse = real_basis(nb, na, chunks, nx)
    cos_y, sin_y = fourier_tables(ny)
    cos_z, sin_z = fourier_tables(nzg)
    table_y = np.block([[cos_y, -sin_y], [sin_y, cos_y]])
    in_plane = [derivative_table(nx).astype(np.float64), derivative_table(ny).T.astype(np.float64)]
    fetched = (
        density[0],
        coef,
        local_factor,
        beside(basis),
        beside(inverse),
        host_split(table_y),
        host_split(derivative_table(nzg).astype(np.float64)),
        host_split(np.concatenate([cos_z, sin_z]) / (nzg * nx * ny)),
        host_split(np.stack(in_plane)),
        pairs,
        miller,
    )

    stress, kinetic_density, square = pl.pallas_call(
        functools.partial(main_kernel, nb, ns, fold_y, fold_z),
        out_shape=(f32(1, 128), f32(rows, 128), f32(zl, nx, ny)),
        in_specs=[pl.BlockSpec(memory_space=pltpu.SMEM)]
        + [pl.BlockSpec(memory_space=pltpu.HBM)] * len(fetched),
        out_specs=(VMEM,) * 3,
        scratch_shapes=[pltpu.VMEM(value.shape, value.dtype) for value in fetched]
        + [
            pltpu.VMEM(shape, jnp.float32)
            for shape in (
                (fold_z * fold_y, 2, ns, rows, 128),
                (chunks, nb * na * block, ny),
                (chunks, ns, nb, block, ny),
                (chunks, ns, hb, block, ny),
                (chunks * hb * na * block, ny),
                (fold_z * fold_y, ns, rows, 128),
                (fold_z, fold_y, ns, rows, 128),
                (fold_y * ns - 1, fold_z, rows, 128),
                (fold_z, rows, 128),
                (fold_z - 1, rows, 128),
                (per, nzg, ny),
                (zl, nx, ny),
                (zl, nx, ny),
                (8, 128),
                (1, 128),
                (nb * ns - 1, 1, 128),
            )
        ]
        + [dma((len(fetched),))]
        + [
            dma(shape)
            for shape in (
                (chunks, nb * ns - 1), (1,), (fold_y * ns - 1,), (fold_z - 1,),
                (chunks, hb * ns - 1), (nb * ns - 1,),
            )
            for _ in range(2)
        ],
        compiler_params=params(0),
        name="main_exchange",
    )(occupation, *fetched)
    return (
        stress[0, :6],
        kinetic_density.reshape(rows * 128),
        square[None],
    )


def solution(mesh):
    return jax.shard_map(
        functools.partial(shards, mesh.shape["band"], mesh.shape["spin"]),
        mesh=mesh,
        in_specs=(
            P("spin", None, "band", None),
            P("spin", "band"),
            P(None, ("band", "spin")),
            P("spin", "band", None, None),
            P(None, None, "band", None),
        ),
        out_specs=(P(), P(("band", "spin")), P("spin", "band", None, None)),
        check_vma=False,
    )
```

```python
import functools

import jax
import jax.numpy as jnp
import numpy as np
from jax import lax
from jax.experimental import pallas as pl
from jax.experimental.pallas import tpu as pltpu
from jax.sharding import PartitionSpec as P

occupation_unit = 1000.0
kpoint = (0.25, 0.125, 0.375)
spacing = 0.25
MESH = pl.DeviceIdType.MESH
VMEM = pl.BlockSpec(memory_space=pltpu.VMEM)
CHUNKS = 4


def derivative_table(length):
    index = np.arange(length)
    wrapped = np.mod(index[:, None] - index[None, :], length)
    angles = np.pi / length * wrapped
    sines = np.where(wrapped == 0, 1.0, np.sin(angles))
    parity = 1.0 - 2.0 * np.mod(wrapped, 2)
    table = np.where(wrapped == 0, 0.0, 0.5 * parity * np.cos(angles) / sines)
    return table.astype(np.float32)


def fourier_tables(length):
    index = np.arange(length)
    phases = np.mod(index[:, None] * index[None, :], length) * (2.0 * np.pi / length)
    return np.cos(phases), np.sin(phases)


def greet_all(nb, ns):
    b, s = lax.axis_index("band"), lax.axis_index("spin")
    barrier = pltpu.get_barrier_semaphore()

    def greet(k):
        offset = far_first(k, nb * ns)
        pl.semaphore_signal(
            barrier,
            inc=1,
            device_id=((b + offset // ns) % nb, (s + offset % ns) % ns),
            device_id_type=MESH,
        )

    loop(0, nb * ns - 1, greet)
    return b, s


def far_first(k, count):
    return 1 + (k + count // 2 - 1) % (count - 1)


def split(value):
    high = value.astype(jnp.bfloat16)
    return high, (value - high.astype(jnp.float32)).astype(jnp.bfloat16)


def host_split(table):
    high = table.astype(np.float32).astype(jnp.bfloat16)
    low = (table - high.astype(np.float64)).astype(np.float32).astype(jnp.bfloat16)
    return np.stack([high, low])


def dot3(left, right):
    def one(p, q):
        return jnp.dot(p, q, preferred_element_type=jnp.float32)

    return one(left[0], right[0]) + (one(left[0], right[1]) + one(left[1], right[0]))


def loop(low, high, step):
    def body(k, carry):
        step(k)
        return carry

    lax.fori_loop(low, high, body, 0)


def axis_frequency(index, length):
    signed = jnp.where(index >= length // 2, index - length, index)
    return 2.0 * np.pi / length * signed.astype(jnp.float32)


def fold(value):
    return jnp.sum(value, axis=0, keepdims=True)


def guard(always, condition, step):
    if always:
        step()
    else:
        pl.when(condition)(step)


def stack3(left, right):
    high, low = right
    depth = high.shape[0]
    return jnp.dot(
        left, jnp.concatenate([high, high], axis=0), preferred_element_type=jnp.float32
    ) + jnp.dot(left[:, :depth], low, preferred_element_type=jnp.float32)


def main_kernel(
    nb, ns, ny, nz, occupation, dens_h, coef_h, factor_h,
    table_f_h, table_i_h, table_y_h, table_d_h, table_z_h, table_g_h, pairs_h, miller_h,
    stress, kdens, square,
    dens, coef, factor, table_f, table_i, table_y, table_d, table_z, table_g, pairs, miller,
    kin, out, col, grad, gout, from_core, sum_core, from_plane, sum_plane, from_line,
    inverses, grad_x, grad_y, above, slopes, tally, part, row, held,
    f_sem, d_send, d_recv, c_send, c_recv, p_send, p_recv, l_send, l_recv,
    g_send, g_recv, t_send, t_recv,
):
    sources = (dens_h, table_f_h, coef_h, pairs_h, table_g_h, table_d_h, table_y_h, table_z_h, factor_h, table_i_h, miller_h)
    targets = (dens, table_f, coef, pairs, table_g, table_d, table_y, table_z, factor, table_i, miller)
    fetches = [
        pltpu.make_async_copy(source, target, f_sem.at[i])
        for i, (source, target) in enumerate(zip(sources, targets))
    ]
    for fetch in fetches[:2]:
        fetch.start()
    b, s = greet_all(nb, ns)
    n = nb * ns
    core, y, z = b % 2, (b // 2) % ny, b // (2 * ny)
    zl, nx, width = dens.shape
    chunks, _, _, block, _ = col.shape
    hb = nb // 2
    half, u = b // hb, b % hb
    xl = nx // nb
    na = min(ns, xl)
    per = xl // na
    each = per // chunks
    rc = 2 * each
    zp = block // rc
    hz = hb * zl
    nzg = nb * zl
    rows = kdens.shape[0]
    whole, mine = na == ns, s < na
    for fetch in fetches[:2]:
        fetch.wait()
    for fetch in fetches[2:]:
        fetch.start()

    def peer(k, count):
        offset = far_first(k, count * ns)
        return (offset // ns, (s + offset % ns) % ns)

    def block_copy(c, k):
        step, ts = peer(k, nb)
        tb = (b + step) % nb
        at = pl.multiple_of((tb * na + ts) * block, block)
        return ts < na, pltpu.make_async_remote_copy(
            out.at[c, pl.ds(at, block), :], col.at[c, s, b], d_send.at[c, k], d_recv.at[c, k],
            device_id=(tb, ts), device_id_type=MESH,
        )

    def forward(i, which):
        value = split(jnp.concatenate([dens[2 * i], dens[2 * i + 1]], axis=1))
        for c in which:
            turned = stack3(table_f[c], value)
            out[c, pl.ds(2 * i, nb * na * rc, stride=zp), :] = turned[:, :width]
            out[c, pl.ds(2 * i + 1, nb * na * rc, stride=zp), :] = turned[:, width:]

    def send_chunk(c):
        def send(k):
            right, copy = block_copy(c, k)
            guard(whole, right, copy.start)

        loop(0, n - 1, send)

        def keep():
            at = pl.multiple_of((b * na + s) * block, block)
            col[c, s, b] = out[c, pl.ds(at, block), :]

        guard(whole, mine, keep)

    def forward_first(i):
        forward(i, range(1))

    def forward_rest(i):
        forward(i, range(1, chunks))

    loop(0, zl // 2, forward_first)
    pl.semaphore_wait(pltpu.get_barrier_semaphore(), n - 1)
    send_chunk(0)
    if chunks > 1:
        loop(0, zl // 2, forward_rest)
    for c in range(1, chunks):
        send_chunk(c)

    nbl = occupation.shape[1]
    depth = rows * nbl
    band = lax.broadcasted_iota(jnp.int32, (depth, 128), 0) % nbl
    weight = jnp.zeros((depth, 128), jnp.float32)
    for j in range(nbl):
        share = jnp.full((depth, 128), occupation[0, j]).astype(jnp.float32) / occupation_unit
        weight = jnp.where(band == j, share, weight)
    for fetch in fetches[2:4]:
        fetch.wait()

    def kinetic(i):
        here = pl.ds(pl.multiple_of(i * depth, depth), depth)
        real, imag = coef[0, here, :].astype(jnp.float32), coef[1, here, :].astype(jnp.float32)
        high, low = split(weight * (real * real + imag * imag))
        kin[i // (2 * ns), (i // ns) % 2, i % ns] = jnp.dot(
            pairs[...], high, preferred_element_type=jnp.float32
        ) + jnp.dot(pairs[...], low, preferred_element_type=jnp.float32)

    loop(0, n, kinetic)
    core_copy = pltpu.make_async_remote_copy(
        kin.at[:, 1 - core], from_core, c_send.at[0], c_recv.at[0],
        device_id=(b + 1 - 2 * core, s), device_id_type=MESH,
    )
    core_copy.start()

    fetches[4].wait()

    def in_plane(i):
        value = split(dens[i])
        grad_x[i] = dot3((table_g[0, 0], table_g[1, 0]), value)
        grad_y[i] = dot3(value, (table_g[0, 1], table_g[1, 1]))
        scale = 4.0 * dens[i] * dens[i] + 1.0
        weigh = jnp.exp(jnp.log(dens[i]) * (-1.0 / 3.0)) * scale
        above[i] = weigh * (-1.0 / (nzg * nx * width))

    loop(0, zl, in_plane)

    core_copy.wait()

    def add_core(i):
        sum_core[i // ny, i % ny] = kin[i, core] + from_core[i]

    loop(0, nz * ny, add_core)
    plane_copies = []
    for k in range(1, ny * ns):
        ty, ts = (y + k // ns) % ny, (s + k % ns) % ns
        copy = pltpu.make_async_remote_copy(
            sum_core.at[:, ty, ts], from_plane.at[k - 1], p_send.at[k - 1], p_recv.at[k - 1],
            device_id=((z * ny + ty) * 2 + core, ts), device_id_type=MESH,
        )
        copy.start()
        plane_copies.append(copy)

    freq_z = axis_frequency(lax.broadcasted_iota(jnp.int32, (nzg, width), 0), nzg)
    freq_y = axis_frequency(lax.broadcasted_iota(jnp.int32, (nzg, width), 1), width)
    row_y = freq_y[:1]

    def place(j):
        return b * xl + s * per + j

    def invert(j):
        freq_x = axis_frequency(jnp.full((nzg, width), place(j)), nx)
        length = freq_x * freq_x + freq_y * freq_y + freq_z * freq_z
        positive = length > 0
        inverses[j] = jnp.where(positive, 1.0 / jnp.where(positive, length, 1.0), 0.0)

    loop(0, per, invert)

    part[...] = jnp.zeros_like(part)
    tally[...] = jnp.zeros_like(tally)
    for fetch in fetches[5:10]:
        fetch.wait()

    def back_copy(c, k):
        step, ts = peer(k, hb)
        tu = (u + step) % hb
        at = pl.multiple_of(((c * hb + u) * na + s) * block, block)
        return (s - (ts - s)) % ns < na, pltpu.make_async_remote_copy(
            grad.at[c, ts, tu], gout.at[pl.ds(at, block), :], g_send.at[c, k], g_recv.at[c, k],
            device_id=(half * hb + tu, ts), device_id_type=MESH,
        )

    def column(c, k, r):
        return col[c, k, :, pl.ds(pl.multiple_of(r * zp, zp), zl), :].reshape(nzg, width)

    def line_copy(k):
        tz = (z + k) % nz
        return pltpu.make_async_remote_copy(
            sum_plane.at[tz], from_line.at[k - 1], l_send.at[k - 1], l_recv.at[k - 1],
            device_id=((tz * ny + y) * 2 + core, s), device_id_type=MESH,
        )

    def finish_planes():
        for copy in plane_copies:
            copy.wait()
        total = sum_core[:, y, s]
        for k in range(1, ny * ns):
            total = total + from_plane[k - 1]
        sum_plane[...] = total
        loop(1, nz, lambda k: line_copy(k).start())

    def gather_back(c):
        def collect(k):
            right, copy = back_copy(c, k)
            guard(whole, mine, copy.wait_send)
            guard(whole, right, copy.wait_recv)

        loop(0, hb * ns - 1, collect)

    def returned(c, i):
        count = hb * na * rc
        high, low = split(
            jnp.concatenate(
                [
                    gout[pl.ds(c * count * zp + 2 * i + j, count, stride=zp), :]
                    for j in range(2)
                ],
                axis=1,
            )
        )
        return jnp.dot(
            table_i[half, c], jnp.concatenate([high, low, high], axis=0),
            preferred_element_type=jnp.float32,
        )

    def invert_chunk(c, i):
        value = returned(c, i)
        for j in range(2):
            here = value[:, j * width:(j + 1) * width]
            slopes[2 * i + j] = here if c == 0 else slopes[2 * i + j] + here

    rows_d = pl.ds(pl.multiple_of(half * hz, hz), hz)
    for c in range(chunks):

        def receive(k):
            right, copy = block_copy(c, k)
            guard(whole, right, copy.wait_send)
            guard(whole, mine, copy.wait_recv)

        loop(0, n - 1, receive)

        def derive(j):
            k, r = j // each, 2 * (j % each)
            value = split(jnp.concatenate([column(c, k, r), column(c, k, r + 1)], axis=1))
            slope = dot3((table_d[0, rows_d, :], table_d[1, rows_d, :]), value)
            for i in range(2):
                here = pl.ds(pl.multiple_of((r + i) * zp, zp), zl)
                grad[c, k, :, here, :] = slope[:, i * width:(i + 1) * width].reshape(hb, zl, width)

        def give_back(k):
            back_copy(c, k)[1].start()

        def local_back():
            at = pl.multiple_of(((c * hb + u) * na + s) * block, block)
            gout[pl.ds(at, block), :] = grad[c, s, u]

        def transform(i):
            j = c * each + i
            real, imag = column(c, 0, i), column(c, 0, each + i)
            for k in range(1, ns):
                real, imag = real + column(c, k, i), imag + column(c, k, each + i)
            position = jnp.full((nzg, width), place(j))
            imag = jnp.where(position % (nx // 2) == 0, 0.0, imag)
            value = split(jnp.concatenate([real, imag], axis=1))
            value = split(dot3(value, (table_y[0], table_y[1])))
            turned = dot3((table_z[0], table_z[1]), value)
            real = turned[:nzg, :width] + turned[nzg:, width:]
            imag = turned[:nzg, width:] - turned[nzg:, :width]
            inverse = inverses[j]
            here = s * per + j
            local = real * factor[0, :, here, :] + imag * factor[1, :, here, :]
            hartree = (4.0 * np.pi) * (real * real + imag * imag) * inverse
            weigh = 2.0 * (hartree * inverse + local)
            weigh_z = weigh * freq_z
            plain, along_z, along_zz = fold(weigh), fold(weigh_z), fold(weigh_z * freq_z)
            trace = fold(hartree)
            row_x = axis_frequency(position[:1], nx)
            terms = (
                plain * row_x * row_x - trace,
                plain * row_y * row_y - trace,
                along_zz - trace,
                along_z * row_y,
                along_z * row_x,
                plain * row_x * row_y,
            )
            for i, term in enumerate(terms):
                part[pl.ds(i, 1), :] += term

        def work():
            loop(0, ns * each, derive)
            loop(0, hb * ns - 1, give_back)
            local_back()
            loop(0, each, transform)

        guard(whole, mine, work)
        if c == max(chunks - 2, 0):
            finish_planes()
        if c > 0:
            gather_back(c - 1)
            loop(0, zl // 2, functools.partial(invert_chunk, c - 1))

    loop(1, nz, lambda k: line_copy(k).wait())
    kweight = sum_plane[z] + jnp.sum(from_line[...], axis=0)
    fetches[10].wait()
    gk = [spacing * (miller[i].reshape(rows, 128).astype(jnp.float32) + kpoint[i]) for i in range(3)]
    kdens[...] = 0.5 * (gk[0] * gk[0] + gk[1] * gk[1] + gk[2] * gk[2]) * kweight
    scaled = kweight * (-1.0 / (n * rows * 128))
    order = ((0, 0), (1, 1), (2, 2), (1, 2), (0, 2), (0, 1))
    for i, (p, q) in enumerate(order):
        part[pl.ds(i, 1), :] += fold(scaled * gk[p] * gk[q])

    gather_back(chunks - 1)

    def exchange(i):
        last = returned(chunks - 1, i)
        tallies = [tally[t] for t in range(len(order))]
        for j in range(2):
            here = last[:, j * width:(j + 1) * width]
            if chunks > 1:
                here = here + slopes[2 * i + j]
            g = (grad_x[2 * i + j], grad_y[2 * i + j], here)
            total = g[0] * g[0] + g[1] * g[1] + g[2] * g[2]
            square[2 * i + j] = total
            value = dens[2 * i + j]
            weigh = above[2 * i + j] / (4.0 * value * value + 1.0 + total)
            scaled = [weigh * g[p] for p in range(3)]
            for t, (p, q) in enumerate(order):
                term = (scaled[p] * g[q]).reshape(nx // 8, 8, width)
                tallies[t] = tallies[t] + jnp.sum(term, axis=0)
        for t in range(len(order)):
            tally[t] = tallies[t]

    loop(0, zl // 2, exchange)
    for t in range(len(order)):
        part[pl.ds(t, 1), :] += fold(tally[t])
    spots = [lax.broadcasted_iota(jnp.int32, (8, 128), i) for i in range(2)]
    sums = jnp.sum(part[...], axis=1, keepdims=True)
    row[...] = fold(jnp.where(spots[0] == spots[1], sums, 0.0))

    def stress_copy(k):
        step, ts = peer(k, nb)
        return pltpu.make_async_remote_copy(
            row, held.at[k], t_send.at[k], t_recv.at[k],
            device_id=((b + step) % nb, ts), device_id_type=MESH,
        )

    def share_stress(k):
        stress_copy(k).start()

    def wait_stress(k):
        stress_copy(k).wait()

    loop(0, n - 1, share_stress)
    loop(0, n - 1, wait_stress)
    stress[...] = row[...] + jnp.sum(held[...], axis=0)


def params(number):
    return pltpu.CompilerParams(
        collective_id=number, has_side_effects=True, vmem_limit_bytes=60 * 2**20
    )


def f32(*shape):
    return jax.ShapeDtypeStruct(shape, jnp.float32)


def real_basis(nb, na, chunks, nx):
    xl = nx // nb
    per = xl // na
    each = per // chunks
    x = np.arange(nx)
    basis = np.zeros((chunks, nb, na, 2, each, nx))
    share = np.zeros((chunks, nb, na, 2, each))
    for b in range(nb):
        for j in range(xl):
            k = b * xl + j
            phases = (2.0 * np.pi / nx) * ((k * x) % nx)
            spot = (j % per // each, b, j // per, slice(None), j % each)
            if k % (nx // 2) == 0:
                other = (2.0 * np.pi / nx) * (((nx // 2 - k) * x) % nx)
                basis[spot] = np.stack([np.cos(phases), np.cos(other)])
                share[spot] = 1.0 / nx
            else:
                basis[spot] = np.stack([np.cos(phases), -np.sin(phases)])
                share[spot] = 2.0 / nx
    inverse = (basis * share[..., None]).reshape(chunks, 2, -1, nx)
    inverse = inverse.transpose(1, 0, 3, 2)
    return basis.reshape(chunks, -1, nx), inverse


def beside(table):
    return np.concatenate(list(host_split(table)), axis=-1)


def shards(nb, ns, coefficients, occupation, miller, density, local_factor):
    dma = pltpu.SemaphoreType.DMA
    _, zl, nx, ny = density.shape
    nzg = zl * nb
    xl = nx // nb
    na = min(ns, xl)
    per = xl // na
    chunks = min(CHUNKS, per)
    rc = 2 * (per // chunks)
    zp = zl
    while rc * zp % 8:
        zp += 1
    block = rc * zp
    npw = coefficients.shape[3]
    rows = npw // (nb * ns * 128)
    nbl = coefficients.shape[2]
    fold_y = 2 if nb % 4 == 0 else 1
    fold_z = nb // (2 * fold_y)
    hb = nb // 2

    coef = coefficients[0].reshape(2, nbl, npw // 128, 128)
    coef = coef.transpose(0, 2, 1, 3).reshape(2, npw // 128 * nbl, 128)
    pairs = jnp.asarray(np.kron(np.eye(rows), np.ones((1, nbl))), jnp.bfloat16)
    basis, inverse = real_basis(nb, na, chunks, nx)
    cos_y, sin_y = fourier_tables(ny)
    cos_z, sin_z = fourier_tables(nzg)
    table_y = np.block([[cos_y, -sin_y], [sin_y, cos_y]])
    in_plane = [derivative_table(nx).astype(np.float64), derivative_table(ny).T.astype(np.float64)]
    fetched = (
        density[0],
        coef,
        local_factor,
        beside(basis),
        np.concatenate([host_split(inverse)[k] for k in (0, 0, 1)], axis=-1),
        host_split(table_y),
        host_split(derivative_table(nzg).astype(np.float64)),
        host_split(np.concatenate([cos_z, sin_z]) / (nzg * nx * ny)),
        host_split(np.stack(in_plane)),
        pairs,
        miller,
    )

    stress, kinetic_density, square = pl.pallas_call(
        functools.partial(main_kernel, nb, ns, fold_y, fold_z),
        out_shape=(f32(1, 128), f32(rows, 128), f32(zl, nx, ny)),
        in_specs=[pl.BlockSpec(memory_space=pltpu.SMEM)]
        + [pl.BlockSpec(memory_space=pltpu.HBM)] * len(fetched),
        out_specs=(VMEM,) * 3,
        scratch_shapes=[pltpu.VMEM(value.shape, value.dtype) for value in fetched]
        + [
            pltpu.VMEM(shape, jnp.float32)
            for shape in (
                (fold_z * fold_y, 2, ns, rows, 128),
                (chunks, nb * na * block, ny),
                (chunks, ns, nb, block, ny),
                (chunks, ns, hb, block, ny),
                (chunks * hb * na * block, ny),
                (fold_z * fold_y, ns, rows, 128),
                (fold_z, fold_y, ns, rows, 128),
                (fold_y * ns - 1, fold_z, rows, 128),
                (fold_z, rows, 128),
                (fold_z - 1, rows, 128),
                (per, nzg, ny),
                (zl, nx, ny),
                (zl, nx, ny),
                (zl, nx, ny),
                (zl, nx, ny),
                (6, 8, ny),
                (8, 128),
                (1, 128),
                (nb * ns - 1, 1, 128),
            )
        ]
        + [dma((len(fetched),))]
        + [
            dma(shape)
            for shape in (
                (chunks, nb * ns - 1), (1,), (fold_y * ns - 1,), (fold_z - 1,),
                (chunks, hb * ns - 1), (nb * ns - 1,),
            )
            for _ in range(2)
        ],
        compiler_params=params(0),
        name="main_exchange",
    )(occupation, *fetched)
    return (
        stress[0, :6],
        kinetic_density.reshape(rows * 128),
        square[None],
    )


def solution(mesh):
    return jax.shard_map(
        functools.partial(shards, mesh.shape["band"], mesh.shape["spin"]),
        mesh=mesh,
        in_specs=(
            P("spin", None, "band", None),
            P("spin", "band"),
            P(None, ("band", "spin")),
            P("spin", "band", None, None),
            P(None, None, "band", None),
        ),
        out_specs=(P(), P(("band", "spin")), P("spin", "band", None, None)),
        check_vma=False,
    )
```

```python
import functools

import jax
import jax.numpy as jnp
import numpy as np
from jax import lax
from jax.experimental import pallas as pl
from jax.experimental.pallas import tpu as pltpu
from jax.sharding import PartitionSpec as P

occupation_unit = 1000.0
kpoint = (0.25, 0.125, 0.375)
spacing = 0.25
MESH = pl.DeviceIdType.MESH
CHUNKS = 4
AHEAD = 2


def derivative_table(length):
    index = np.arange(length)
    wrapped = np.mod(index[:, None] - index[None, :], length)
    angles = np.pi / length * wrapped
    sines = np.where(wrapped == 0, 1.0, np.sin(angles))
    parity = 1.0 - 2.0 * np.mod(wrapped, 2)
    table = np.where(wrapped == 0, 0.0, 0.5 * parity * np.cos(angles) / sines)
    return table.astype(np.float32)


def fourier_tables(length):
    index = np.arange(length)
    phases = np.mod(index[:, None] * index[None, :], length) * (2.0 * np.pi / length)
    return np.cos(phases), np.sin(phases)


def wrapped(value, count):
    return jnp.where(value >= count, value - count, value)


def far_first(count, step):
    loop(count // 2, count, step)
    loop(1, count // 2, step)


def partner(b, s, offset, nb, ns):
    hop = lax.div(offset, ns)
    return wrapped(b + hop, nb), wrapped(s + offset - hop * ns, ns)


def greet_all(nb, ns):
    b, s = lax.axis_index("band"), lax.axis_index("spin")
    barrier = pltpu.get_barrier_semaphore()

    def greet(k):
        pl.semaphore_signal(
            barrier, inc=1, device_id=partner(b, s, k, nb, ns), device_id_type=MESH
        )

    far_first(nb * ns, greet)
    return b, s


def split(value):
    high = value.astype(jnp.bfloat16)
    return high, (value - high.astype(jnp.float32)).astype(jnp.bfloat16)


def host_split(table):
    high = table.astype(np.float32).astype(jnp.bfloat16)
    low = (table - high.astype(np.float64)).astype(np.float32).astype(jnp.bfloat16)
    return np.stack([high, low])


def dot3(left, right):
    def one(p, q):
        return jnp.dot(p, q, preferred_element_type=jnp.float32)

    return one(left[0], right[0]) + (one(left[0], right[1]) + one(left[1], right[0]))


def loop(low, high, step):
    def body(k, carry):
        step(k)
        return carry

    lax.fori_loop(low, high, body, 0)


def axis_frequency(index, length):
    signed = jnp.where(index >= length // 2, index - length, index)
    return 2.0 * np.pi / length * signed.astype(jnp.float32)


def fold(value):
    return jnp.sum(value, axis=0, keepdims=True)


def guard(always, condition, step):
    if always:
        step()
    else:
        pl.when(condition)(step)


def stack3(left, right):
    high, low = right
    depth = high.shape[0]
    return jnp.dot(
        left, jnp.concatenate([high, high], axis=0), preferred_element_type=jnp.float32
    ) + jnp.dot(left[:, :depth], low, preferred_element_type=jnp.float32)


def settle(ref, semaphore):
    pltpu.make_async_copy(ref, ref, semaphore).wait()


def main_kernel(
    nb, ns, ny, nz, occupation, dens_h, coef_h, factor_h,
    table_f_h, table_i_h, table_y_h, table_d_h, table_z_h, table_g_h, miller_h,
    stress_o, kdens_o, square_o,
    dens, coef, factor, table_f, table_i, table_y, table_d, table_z, table_g, miller,
    stress, kdens, square, squares, kin, out, col, grad, gout, from_core, sum_core, from_plane, sum_plane, from_line, pair, from_pair,
    inverses, grad_x, grad_y, above, slopes, tally, part, row, held,
    f_sem, o_sem, d_send, d_recv, c_send, c_recv, p_send, p_recv, l_send, l_recv, x_send, x_recv,
    g_send, g_recv, t_send, t_recv,
):
    sources = (dens_h, table_f_h, coef_h, table_g_h, table_d_h, table_y_h, table_z_h, factor_h, table_i_h, miller_h)
    targets = (dens, table_f, coef, table_g, table_d, table_y, table_z, factor, table_i, miller)
    fetches = [
        pltpu.make_async_copy(source, target, f_sem.at[i])
        for i, (source, target) in enumerate(zip(sources, targets))
    ]
    for fetch in fetches[:2]:
        fetch.start()
    b, s = greet_all(nb, ns)
    n = nb * ns
    core, y, z = b % 2, (b // 2) % ny, b // (2 * ny)
    zl, nx, width = dens.shape
    chunks, _, _, block, _ = col.shape
    hb = nb // 2
    half, u = b // hb, b % hb
    xl = nx // nb
    na = min(ns, xl)
    per = xl // na
    each = per // chunks
    rc = 2 * each
    zp = block // rc
    hz = hb * zl
    nzg = nb * zl
    rows = kdens.shape[0]
    whole, mine = na == ns, s < na
    for fetch in fetches[:2]:
        fetch.wait()
    for fetch in fetches[2:]:
        fetch.start()

    def block_copy(c, k):
        tb, ts = partner(b, s, k, nb, ns)
        at = pl.multiple_of((tb * na + ts) * block, block)
        return ts < na, pltpu.make_async_remote_copy(
            out.at[c, pl.ds(at, block), :], col.at[c, s, b], d_send.at[c], d_recv.at[c],
            device_id=(tb, ts), device_id_type=MESH,
        )

    def forward(i, which):
        value = split(jnp.concatenate([dens[2 * i], dens[2 * i + 1]], axis=1))
        for c in which:
            turned = stack3(table_f[c], value)
            out[c, pl.ds(2 * i, nb * na * rc, stride=zp), :] = turned[:, :width]
            out[c, pl.ds(2 * i + 1, nb * na * rc, stride=zp), :] = turned[:, width:]

    def send_chunk(c):
        def send(k):
            right, copy = block_copy(c, k)
            guard(whole, right, copy.start)

        far_first(n, send)

        def keep():
            at = pl.multiple_of((b * na + s) * block, block)
            pltpu.make_async_copy(out.at[c, pl.ds(at, block), :], col.at[c, s, b], d_recv.at[c]).start()

        guard(whole, mine, keep)

    def forward_first(i):
        forward(i, range(1))

    def forward_rest(i):
        forward(i, range(1, chunks))

    loop(0, zl // 2, forward_first)
    pl.semaphore_wait(pltpu.get_barrier_semaphore(), n - 1)
    send_chunk(0)

    nbl = occupation.shape[1]
    depth = rows * nbl
    shares = [
        jnp.full((rows, 128), occupation[0, j]).astype(jnp.float32) / occupation_unit
        for j in range(nbl)
    ]
    fetches[2].wait()

    def kinetic(i):
        for j in range(2):
            k = 2 * i + j
            here = pl.ds(pl.multiple_of(k * depth, depth), depth)
            real, imag = coef[0, here, :].astype(jnp.float32), coef[1, here, :].astype(jnp.float32)
            squares[j] = real * real + imag * imag
            total = shares[0] * squares[j, pl.ds(0, rows, stride=nbl), :]
            for m in range(1, nbl):
                total = total + shares[m] * squares[j, pl.ds(m, rows, stride=nbl), :]
            kin[lax.div(k, 2 * ns), lax.rem(lax.div(k, ns), 2), lax.rem(k, ns)] = total

    loop(0, n // 2, kinetic)
    core_copy = pltpu.make_async_remote_copy(
        kin.at[:, 1 - core], from_core, c_send.at[0], c_recv.at[0],
        device_id=(b + 1 - 2 * core, s), device_id_type=MESH,
    )
    core_copy.start()
    if chunks > 1:
        loop(0, zl // 2, forward_rest)
    core_copy.wait()

    def add_core(i):
        sum_core[lax.div(i, ny), lax.rem(i, ny)] = kin[i, core] + from_core[i]

    loop(0, nz * ny, add_core)
    plane_copies = []
    for k in range(1, ny * ns):
        ty, ts = (y + k // ns) % ny, (s + k % ns) % ns
        copy = pltpu.make_async_remote_copy(
            sum_core.at[:, ty, ts], from_plane.at[k - 1], p_send.at[k - 1], p_recv.at[k - 1],
            device_id=((z * ny + ty) * 2 + core, ts), device_id_type=MESH,
        )
        copy.start()
        plane_copies.append(copy)
    for c in range(1, min(AHEAD, chunks)):
        send_chunk(c)

    fetches[3].wait()

    def in_plane(i):
        value = split(dens[i])
        grad_x[i] = dot3((table_g[0, 0], table_g[1, 0]), value)
        grad_y[i] = dot3(value, (table_g[0, 1], table_g[1, 1]))
        scale = 4.0 * dens[i] * dens[i] + 1.0
        weigh = jnp.exp(jnp.log(dens[i]) * (-1.0 / 3.0)) * scale
        above[i] = weigh * (-1.0 / (nzg * nx * width))

    loop(0, zl, in_plane)

    freq_z = axis_frequency(lax.broadcasted_iota(jnp.int32, (nzg, width), 0), nzg)
    freq_y = axis_frequency(lax.broadcasted_iota(jnp.int32, (nzg, width), 1), width)
    row_y = freq_y[:1]

    def place(j):
        return b * xl + s * per + j

    def invert(j):
        freq_x = axis_frequency(jnp.full((nzg, width), place(j)), nx)
        length = freq_x * freq_x + freq_y * freq_y + freq_z * freq_z
        positive = length > 0
        inverses[j] = jnp.where(positive, 1.0 / jnp.where(positive, length, 1.0), 0.0)

    loop(0, per, invert)

    part[...] = jnp.zeros_like(part)
    tally[...] = jnp.zeros_like(tally)
    for fetch in fetches[4:9]:
        fetch.wait()

    def back_copy(c, k):
        tu, ts = partner(u, s, k, hb, ns)
        at = pl.multiple_of(((c * hb + u) * na + s) * block, block)
        return wrapped(2 * s - ts + ns, ns) < na, pltpu.make_async_remote_copy(
            grad.at[c, ts, tu], gout.at[pl.ds(at, block), :], g_send.at[c], g_recv.at[c],
            device_id=(half * hb + tu, ts), device_id_type=MESH,
        )

    def column(c, k, r):
        return col[c, k, :, pl.ds(pl.multiple_of(r * zp, zp), zl), :].reshape(nzg, width)

    nh = nz // 2
    zhalf, zin = z // nh, z % nh

    def line_copy(k):
        tz = (zin + k) % nh
        return pltpu.make_async_remote_copy(
            sum_plane.at[:, tz], from_line.at[k - 1], l_send.at[k - 1], l_recv.at[k - 1],
            device_id=(((zhalf * nh + tz) * ny + y) * 2 + core, s), device_id_type=MESH,
        )

    cross_copy = pltpu.make_async_remote_copy(
        pair.at[1 - zhalf], from_pair, x_send.at[0], x_recv.at[0],
        device_id=((((1 - zhalf) * nh + zin) * ny + y) * 2 + core, s), device_id_type=MESH,
    )

    def finish_planes():
        for copy in plane_copies:
            copy.wait()
        total = sum_core[:, y, s]
        for k in range(1, ny * ns):
            total = total + from_plane[k - 1]
        sum_plane[...] = total.reshape(2, nh, rows, 128)
        loop(1, nh, lambda k: line_copy(k).start())

    def cross_lines():
        loop(1, nh, lambda k: line_copy(k).wait())
        pair[...] = sum_plane[:, zin] + jnp.sum(from_line[...], axis=0)
        cross_copy.start()

    def gather_back(c):
        count = hb * na * block
        settle(gout.at[pl.ds(c * count, count), :], g_recv.at[c])

    def returned(c, i):
        count = hb * na * rc
        high, low = split(
            jnp.concatenate(
                [
                    gout[pl.ds(c * count * zp + 2 * i + j, count, stride=zp), :]
                    for j in range(2)
                ],
                axis=1,
            )
        )
        return jnp.dot(
            table_i[half, c], jnp.concatenate([high, low, high], axis=0),
            preferred_element_type=jnp.float32,
        )

    def invert_chunk(c, i):
        value = returned(c, i)
        for j in range(2):
            here = value[:, j * width:(j + 1) * width]
            slopes[2 * i + j] = here if c == 0 else slopes[2 * i + j] + here

    rows_d = pl.ds(pl.multiple_of(half * hz, hz), hz)
    for c in range(chunks):

        guard(whole, mine, functools.partial(settle, col.at[c], d_recv.at[c]))

        def derive(j):
            k, r = j // each, 2 * (j % each)
            value = split(jnp.concatenate([column(c, k, r), column(c, k, r + 1)], axis=1))
            slope = dot3((table_d[0, rows_d, :], table_d[1, rows_d, :]), value)
            for i in range(2):
                here = pl.ds(pl.multiple_of((r + i) * zp, zp), zl)
                grad[c, k, :, here, :] = slope[:, i * width:(i + 1) * width].reshape(hb, zl, width)

        def give_back(k):
            back_copy(c, k)[1].start()

        def local_back():
            at = pl.multiple_of(((c * hb + u) * na + s) * block, block)
            pltpu.make_async_copy(grad.at[c, s, u], gout.at[pl.ds(at, block), :], g_recv.at[c]).start()

        def transform(i):
            j = c * each + i
            real, imag = column(c, 0, i), column(c, 0, each + i)
            for k in range(1, ns):
                real, imag = real + column(c, k, i), imag + column(c, k, each + i)
            position = jnp.full((nzg, width), place(j))
            imag = jnp.where(position % (nx // 2) == 0, 0.0, imag)
            value = split(jnp.concatenate([real, imag], axis=1))
            value = split(dot3(value, (table_y[0], table_y[1])))
            turned = dot3((table_z[0], table_z[1]), value)
            real = turned[:nzg, :width] + turned[nzg:, width:]
            imag = turned[:nzg, width:] - turned[nzg:, :width]
            inverse = inverses[j]
            here = s * per + j
            local = real * factor[0, :, here, :] + imag * factor[1, :, here, :]
            hartree = (4.0 * np.pi) * (real * real + imag * imag) * inverse
            weigh = 2.0 * (hartree * inverse + local)
            weigh_z = weigh * freq_z
            plain, along_z, along_zz = fold(weigh), fold(weigh_z), fold(weigh_z * freq_z)
            trace = fold(hartree)
            row_x = axis_frequency(position[:1], nx)
            terms = (
                plain * row_x * row_x - trace,
                plain * row_y * row_y - trace,
                along_zz - trace,
                along_z * row_y,
                along_z * row_x,
                plain * row_x * row_y,
            )
            for i, term in enumerate(terms):
                part[pl.ds(i, 1), :] += term

        def work():
            loop(0, ns * each, derive)
            far_first(hb * ns, give_back)
            local_back()

        def spectrum():
            loop(0, each, transform)

        guard(whole, mine, work)
        if c + AHEAD < chunks:
            send_chunk(c + AHEAD)
        guard(whole, mine, spectrum)
        if c == max(chunks - 3, 0):
            finish_planes()
        if c == max(chunks - 2, 0):
            cross_lines()
        if c > 0:
            gather_back(c - 1)
            loop(0, zl // 2, functools.partial(invert_chunk, c - 1))

    cross_copy.wait()
    kweight = pair[zhalf] + from_pair[...]
    fetches[9].wait()
    gk = [spacing * (miller[i].reshape(rows, 128).astype(jnp.float32) + kpoint[i]) for i in range(3)]
    kdens[...] = 0.5 * (gk[0] * gk[0] + gk[1] * gk[1] + gk[2] * gk[2]) * kweight
    scaled = kweight * (-1.0 / (n * rows * 128))
    order = ((0, 0), (1, 1), (2, 2), (1, 2), (0, 2), (0, 1))
    for i, (p, q) in enumerate(order):
        part[pl.ds(i, 1), :] += fold(scaled * gk[p] * gk[q])

    gather_back(chunks - 1)

    group = 2 if zl % 4 == 0 else 1

    def exchange(i):
        lasts = [returned(chunks - 1, group * i + m) for m in range(group)]
        tallies = [tally[t] for t in range(len(order))]
        for j in range(2 * group):
            spot = 2 * group * i + j
            here = lasts[j // 2][:, j % 2 * width:(j % 2 + 1) * width]
            if chunks > 1:
                here = here + slopes[spot]
            g = (grad_x[spot], grad_y[spot], here)
            total = g[0] * g[0] + g[1] * g[1] + g[2] * g[2]
            square[spot] = total
            value = dens[spot]
            weigh = above[spot] / (4.0 * value * value + 1.0 + total)
            scaled = [weigh * g[p] for p in range(3)]
            for t, (p, q) in enumerate(order):
                term = (scaled[p] * g[q]).reshape(nx // 8, 8, width)
                tallies[t] = tallies[t] + jnp.sum(term, axis=0)
        for t in range(len(order)):
            tally[t] = tallies[t]

    loop(0, zl // (2 * group), exchange)
    for t in range(len(order)):
        part[pl.ds(t, 1), :] += fold(tally[t])
    spots = [lax.broadcasted_iota(jnp.int32, (8, 128), i) for i in range(2)]
    sums = jnp.sum(part[...], axis=1, keepdims=True)
    row[...] = fold(jnp.where(spots[0] == spots[1], sums, 0.0))

    def stress_copy(k):
        return pltpu.make_async_remote_copy(
            row, held.at[k - 1], t_send.at[0], t_recv.at[0],
            device_id=partner(b, s, k, nb, ns), device_id_type=MESH,
        )

    def share_stress(k):
        stress_copy(k).start()

    def drain(c, count, semaphore):
        settle(out.at[c, pl.ds(0, count * block), :], semaphore.at[c])

    results = [
        pltpu.make_async_copy(value, target, o_sem.at[i])
        for i, (value, target) in enumerate(
            ((stress, stress_o), (kdens, kdens_o), (square, square_o))
        )
    ]
    far_first(n, share_stress)
    for result in results[1:]:
        result.start()
    for c in range(chunks):
        guard(whole, mine, functools.partial(drain, c, nb * na - 1, d_send))
        guard(whole, mine, functools.partial(drain, c, hb * ns - 1, g_send))
        if not whole:
            pl.when(s >= na)(functools.partial(drain, c, nb * na, d_send))
    settle(held, t_send.at[0])
    settle(held, t_recv.at[0])
    stress[...] = row[...] + jnp.sum(held[...], axis=0)
    results[0].start()
    for result in results:
        result.wait()


def params(number):
    return pltpu.CompilerParams(
        collective_id=number, has_side_effects=True, vmem_limit_bytes=60 * 2**20
    )


def vmem(*shape):
    return pltpu.VMEM(shape, jnp.float32)


def real_basis(nb, na, chunks, nx):
    xl = nx // nb
    per = xl // na
    each = per // chunks
    x = np.arange(nx)
    basis = np.zeros((chunks, nb, na, 2, each, nx))
    share = np.zeros((chunks, nb, na, 2, each))
    for b in range(nb):
        for j in range(xl):
            k = b * xl + j
            phases = (2.0 * np.pi / nx) * ((k * x) % nx)
            spot = (j % per // each, b, j // per, slice(None), j % each)
            if k % (nx // 2) == 0:
                other = (2.0 * np.pi / nx) * (((nx // 2 - k) * x) % nx)
                basis[spot] = np.stack([np.cos(phases), np.cos(other)])
                share[spot] = 1.0 / nx
            else:
                basis[spot] = np.stack([np.cos(phases), -np.sin(phases)])
                share[spot] = 2.0 / nx
    inverse = (basis * share[..., None]).reshape(chunks, 2, -1, nx)
    inverse = inverse.transpose(1, 0, 3, 2)
    return basis.reshape(chunks, -1, nx), inverse


def beside(table):
    return np.concatenate(list(host_split(table)), axis=-1)


def shards(nb, ns, coefficients, occupation, miller, density, local_factor):
    dma = pltpu.SemaphoreType.DMA
    _, zl, nx, ny = density.shape
    nzg = zl * nb
    xl = nx // nb
    na = min(ns, xl)
    per = xl // na
    chunks = min(CHUNKS, per)
    rc = 2 * (per // chunks)
    zp = zl
    while rc * zp % 8:
        zp += 1
    block = rc * zp
    npw = coefficients.shape[3]
    rows = npw // (nb * ns * 128)
    nbl = coefficients.shape[2]
    fold_y = 2 if nb % 4 == 0 else 1
    fold_z = nb // (2 * fold_y)
    hb = nb // 2

    coef = coefficients[0].reshape(2, nbl, npw // 128, 128)
    coef = coef.transpose(0, 2, 1, 3).reshape(2, npw // 128 * nbl, 128)
    basis, inverse = real_basis(nb, na, chunks, nx)
    cos_y, sin_y = fourier_tables(ny)
    cos_z, sin_z = fourier_tables(nzg)
    table_y = np.block([[cos_y, -sin_y], [sin_y, cos_y]])
    in_plane = [derivative_table(nx).astype(np.float64), derivative_table(ny).T.astype(np.float64)]
    fetched = (
        density[0],
        coef,
        local_factor,
        beside(basis),
        np.concatenate([host_split(inverse)[k] for k in (0, 0, 1)], axis=-1),
        host_split(table_y),
        host_split(derivative_table(nzg).astype(np.float64)),
        host_split(np.concatenate([cos_z, sin_z]) / (nzg * nx * ny)),
        host_split(np.stack(in_plane)),
        miller,
    )

    stress, kinetic_density, square = pl.pallas_call(
        functools.partial(main_kernel, nb, ns, fold_y, fold_z),
        out_shape=(vmem(1, 128), vmem(rows, 128), vmem(zl, nx, ny)),
        in_specs=[pl.BlockSpec(memory_space=pltpu.SMEM)]
        + [pl.BlockSpec(memory_space=pltpu.HBM)] * len(fetched),
        out_specs=(pl.BlockSpec(memory_space=pl.ANY),) * 3,
        scratch_shapes=[pltpu.VMEM(value.shape, value.dtype) for value in fetched]
        + [
            pltpu.VMEM(shape, jnp.float32)
            for shape in (
                (1, 128),
                (rows, 128),
                (zl, nx, ny),
                (2, rows * nbl, 128),
                (fold_z * fold_y, 2, ns, rows, 128),
                (chunks, nb * na * block, ny),
                (chunks, ns, nb, block, ny),
                (chunks, ns, hb, block, ny),
                (chunks * hb * na * block, ny),
                (fold_z * fold_y, ns, rows, 128),
                (fold_z, fold_y, ns, rows, 128),
                (fold_y * ns - 1, fold_z, rows, 128),
                (2, fold_z // 2, rows, 128),
                (fold_z // 2 - 1, 2, rows, 128),
                (2, rows, 128),
                (rows, 128),
                (per, nzg, ny),
                (zl, nx, ny),
                (zl, nx, ny),
                (zl, nx, ny),
                (zl, nx, ny),
                (6, 8, ny),
                (8, 128),
                (1, 128),
                (nb * ns - 1, 1, 128),
            )
        ]
        + [dma((len(fetched),)), dma((3,))]
        + [
            dma(shape)
            for shape in (
                (chunks,), (1,), (fold_y * ns - 1,), (fold_z // 2 - 1,), (1,),
                (chunks,), (1,),
            )
            for _ in range(2)
        ],
        compiler_params=params(0),
        name="main_exchange",
    )(occupation, *fetched)
    return (
        stress[0, :6],
        kinetic_density.reshape(rows * 128),
        square[None],
    )


def solution(mesh):
    return jax.shard_map(
        functools.partial(shards, mesh.shape["band"], mesh.shape["spin"]),
        mesh=mesh,
        in_specs=(
            P("spin", None, "band", None),
            P("spin", "band"),
            P(None, ("band", "spin")),
            P("spin", "band", None, None),
            P(None, None, "band", None),
        ),
        out_specs=(P(), P(("band", "spin")), P("spin", "band", None, None)),
        check_vma=False,
    )
```

```python
import functools

import jax
import jax.numpy as jnp
import numpy as np
from jax import lax
from jax.experimental import pallas as pl
from jax.experimental.pallas import tpu as pltpu
from jax.sharding import PartitionSpec as P

occupation_unit = 1000.0
kpoint = (0.25, 0.125, 0.375)
spacing = 0.25
MESH = pl.DeviceIdType.MESH
CHUNKS = 4
PLAN = (((0, 0), (1, 0)), ((0, 1), (0, 2), (0, 3), (0, 4), (1, 1), (1, 2)), ((1, 3), (1, 4)))


def derivative_table(length):
    index = np.arange(length)
    wrapped = np.mod(index[:, None] - index[None, :], length)
    angles = np.pi / length * wrapped
    sines = np.where(wrapped == 0, 1.0, np.sin(angles))
    parity = 1.0 - 2.0 * np.mod(wrapped, 2)
    table = np.where(wrapped == 0, 0.0, 0.5 * parity * np.cos(angles) / sines)
    return table.astype(np.float32)


def fourier_tables(length):
    index = np.arange(length)
    phases = np.mod(index[:, None] * index[None, :], length) * (2.0 * np.pi / length)
    return np.cos(phases), np.sin(phases)


def wrapped(value, count):
    return jnp.where(value >= count, value - count, value)


def far_first(count, step):
    loop(count // 2, count, step)
    loop(1, count // 2, step)


def partner(b, s, offset, nb, ns):
    hop = lax.div(offset, ns)
    return wrapped(b + hop, nb), wrapped(s + offset - hop * ns, ns)


def greet_all(nb, ns):
    b, s = lax.axis_index("band"), lax.axis_index("spin")
    barrier = pltpu.get_barrier_semaphore()

    def greet(k):
        pl.semaphore_signal(
            barrier, inc=1, device_id=partner(b, s, k, nb, ns), device_id_type=MESH
        )

    far_first(nb * ns, greet)
    return b, s


def split(value):
    high = value.astype(jnp.bfloat16)
    return high, (value - high.astype(jnp.float32)).astype(jnp.bfloat16)


def host_split(table):
    high = table.astype(np.float32).astype(jnp.bfloat16)
    low = (table - high.astype(np.float64)).astype(np.float32).astype(jnp.bfloat16)
    return np.stack([high, low])


def dot3(left, right):
    def one(p, q):
        return jnp.dot(p, q, preferred_element_type=jnp.float32)

    return one(left[0], right[0]) + (one(left[0], right[1]) + one(left[1], right[0]))


def loop(low, high, step):
    def body(k, carry):
        step(k)
        return carry

    lax.fori_loop(low, high, body, 0)


def axis_frequency(index, length):
    signed = jnp.where(index >= length // 2, index - length, index)
    return 2.0 * np.pi / length * signed.astype(jnp.float32)


def fold(value):
    return jnp.sum(value, axis=0, keepdims=True)


def guard(always, condition, step):
    if always:
        step()
    else:
        pl.when(condition)(step)


def stack3(left, right):
    high, low = right
    depth = high.shape[0]
    return jnp.dot(
        left, jnp.concatenate([high, high], axis=0), preferred_element_type=jnp.float32
    ) + jnp.dot(left[:, :depth], low, preferred_element_type=jnp.float32)


def settle(ref, semaphore):
    pltpu.make_async_copy(ref, ref, semaphore).wait()


def main_kernel(
    nb, ns, ny, nz, occupation, dens_h, coef_h, factor_h,
    table_f_h, table_i_h, table_y_h, table_d_h, table_z_h, table_g_h, miller_h,
    stress_o, kdens_o, square_o,
    dens, coef, factor, table_f, table_i, table_y, table_d, table_z, table_g, miller,
    stress, kdens, square, squares, kin, out, col, grad, gout, from_core, sum_core, from_plane, sum_plane, from_line, pair, from_pair,
    inverses, grad_x, grad_y, above, slopes, tally, part, row, held,
    f_sem, o_sem, d_send, d_recv, c_send, c_recv, p_send, p_recv, l_send, l_recv, x_send, x_recv,
    g_send, g_recv, t_send, t_recv,
):
    sources = (dens_h, table_f_h, coef_h, table_g_h, table_d_h, table_y_h, table_z_h, factor_h, table_i_h, miller_h)
    targets = (dens, table_f, coef, table_g, table_d, table_y, table_z, factor, table_i, miller)
    fetches = [
        pltpu.make_async_copy(source, target, f_sem.at[i])
        for i, (source, target) in enumerate(zip(sources, targets))
    ]
    b, s = greet_all(nb, ns)
    for fetch in fetches[:2]:
        fetch.start()
    n = nb * ns
    core, y, z = b % 2, (b // 2) % ny, b // (2 * ny)
    zl, nx, width = dens.shape
    chunks, _, _, block, _ = col.shape
    hb = nb // 2
    half, u = b // hb, b % hb
    xl = nx // nb
    na = min(ns, xl)
    per = xl // na
    each = per // chunks
    rc = 2 * each
    zp = block // rc
    units = [(c, 0, rc) for c in range(chunks - 1)]
    units += [(chunks - 1, 0, each), (chunks - 1, each, each)]
    backs = [(m, c, r * zp, count * zp) for m, (c, r, count) in enumerate(units)]
    if zl % 16 == 0 and each == 1:
        m, c, edge, _ = backs.pop()
        backs += [(m, c, edge, zl // 2), (m, c, edge + zl // 2, zl // 2)]
    hz = hb * zl
    nzg = nb * zl
    rows = kdens.shape[0]
    whole, mine = na == ns, s < na
    for fetch in fetches[:2]:
        fetch.wait()
    for fetch in fetches[2:]:
        fetch.start()

    def block_copy(m, k, cross):
        c, r, count = units[m]
        tu, ts = partner(u, s, k, hb, ns)
        tb = tu + hb * (1 - half if cross else half)
        at = pl.multiple_of((tb * na + ts) * block + r * zp, 8)
        return ts < na, pltpu.make_async_remote_copy(
            out.at[c, pl.ds(at, count * zp), :], col.at[c, s, b, pl.ds(r * zp, count * zp), :],
            d_send.at[m], d_recv.at[m], device_id=(tb, ts), device_id_type=MESH,
        )

    def forward(i, which):
        value = split(jnp.concatenate([dens[2 * i], dens[2 * i + 1]], axis=1))
        for c in which:
            turned = stack3(table_f[c], value)
            out[c, pl.ds(2 * i, nb * na * rc, stride=zp), :] = turned[:, :width]
            out[c, pl.ds(2 * i + 1, nb * na * rc, stride=zp), :] = turned[:, width:]

    def send_part(m, cross):
        def send(k):
            right, copy = block_copy(m, k, cross)
            guard(whole, right, copy.start)

        if cross:
            loop(0, hb * ns, send)
        else:
            far_first(hb * ns, send)

    def send_stage(stage):
        for cross, m in PLAN[stage] if stage < len(PLAN) else ():
            if m < len(units):
                send_part(m, cross)

    def keep(m):
        c, r, count = units[m]
        at = pl.multiple_of((b * na + s) * block + r * zp, 8)
        pltpu.make_async_copy(
            out.at[c, pl.ds(at, count * zp), :], col.at[c, s, b, pl.ds(r * zp, count * zp), :],
            d_recv.at[m],
        ).start()

    def forward_first(i):
        forward(i, range(1))

    def forward_rest(i):
        forward(i, range(1, chunks))

    loop(0, zl // 2, forward_first)
    pl.semaphore_wait(pltpu.get_barrier_semaphore(), n - 1)
    send_stage(0)

    nbl = occupation.shape[1]
    depth = rows * nbl
    shares = [
        jnp.full((rows, 128), occupation[0, j]).astype(jnp.float32) / occupation_unit
        for j in range(nbl)
    ]
    fetches[2].wait()

    def kinetic(i):
        for j in range(2):
            k = 2 * i + j
            here = pl.ds(pl.multiple_of(k * depth, depth), depth)
            real, imag = coef[0, here, :].astype(jnp.float32), coef[1, here, :].astype(jnp.float32)
            squares[j] = real * real + imag * imag
            total = shares[0] * squares[j, pl.ds(0, rows, stride=nbl), :]
            for m in range(1, nbl):
                total = total + shares[m] * squares[j, pl.ds(m, rows, stride=nbl), :]
            kin[lax.div(k, 2 * ns), lax.rem(lax.div(k, ns), 2), lax.rem(k, ns)] = total

    loop(0, n // 2, kinetic)
    core_copy = pltpu.make_async_remote_copy(
        kin.at[:, 1 - core], from_core, c_send.at[0], c_recv.at[0],
        device_id=(b + 1 - 2 * core, s), device_id_type=MESH,
    )
    core_copy.start()
    if chunks > 1:
        loop(0, zl // 2, forward_rest)
    core_copy.wait()

    def add_core(i):
        sum_core[lax.div(i, ny), lax.rem(i, ny)] = kin[i, core] + from_core[i]

    loop(0, nz * ny, add_core)
    plane_copies = []
    for k in range(1, ny * ns):
        ty, ts = (y + k // ns) % ny, (s + k % ns) % ns
        copy = pltpu.make_async_remote_copy(
            sum_core.at[:, ty, ts], from_plane.at[k - 1], p_send.at[k - 1], p_recv.at[k - 1],
            device_id=((z * ny + ty) * 2 + core, ts), device_id_type=MESH,
        )
        copy.start()
        plane_copies.append(copy)
    send_stage(1)
    for m in range(len(units)):
        guard(whole, mine, functools.partial(keep, m))

    fetches[3].wait()

    def in_plane(i):
        value = split(dens[i])
        grad_x[i] = dot3((table_g[0, 0], table_g[1, 0]), value)
        grad_y[i] = dot3(value, (table_g[0, 1], table_g[1, 1]))
        scale = 4.0 * dens[i] * dens[i] + 1.0
        weigh = jnp.exp(jnp.log(dens[i]) * (-1.0 / 3.0)) * scale
        above[i] = weigh * (-1.0 / (nzg * nx * width))

    loop(0, zl, in_plane)

    freq_z = axis_frequency(lax.broadcasted_iota(jnp.int32, (nzg, width), 0), nzg)
    freq_y = axis_frequency(lax.broadcasted_iota(jnp.int32, (nzg, width), 1), width)
    row_y = freq_y[:1]

    def place(j):
        return b * xl + s * per + j

    def invert(j):
        freq_x = axis_frequency(jnp.full((nzg, width), place(j)), nx)
        length = freq_x * freq_x + freq_y * freq_y + freq_z * freq_z
        positive = length > 0
        inverses[j] = jnp.where(positive, 1.0 / jnp.where(positive, length, 1.0), 0.0)

    loop(0, per, invert)

    part[...] = jnp.zeros_like(part)
    tally[...] = jnp.zeros_like(tally)
    for fetch in fetches[4:9]:
        fetch.wait()

    def back_copy(i, k):
        _, c, edge, count = backs[i]
        tu, ts = partner(u, s, k, hb, ns)
        at = pl.multiple_of(((c * hb + u) * na + s) * block + edge, 8)
        return pltpu.make_async_remote_copy(
            grad.at[c, ts, tu, pl.ds(edge, count), :], gout.at[pl.ds(at, count), :],
            g_send.at[i], g_recv.at[i], device_id=(half * hb + tu, ts), device_id_type=MESH,
        )

    def local_back(i):
        _, c, edge, count = backs[i]
        at = pl.multiple_of(((c * hb + u) * na + s) * block + edge, 8)
        pltpu.make_async_copy(
            grad.at[c, s, u, pl.ds(edge, count), :], gout.at[pl.ds(at, count), :], g_recv.at[i]
        ).start()

    def column(c, k, r):
        return col[c, k, :, pl.ds(pl.multiple_of(r * zp, zp), zl), :].reshape(nzg, width)

    nh = nz // 2
    zhalf, zin = z // nh, z % nh

    def line_copy(k):
        tz = (zin + k) % nh
        return pltpu.make_async_remote_copy(
            sum_plane.at[:, tz], from_line.at[k - 1], l_send.at[k - 1], l_recv.at[k - 1],
            device_id=(((zhalf * nh + tz) * ny + y) * 2 + core, s), device_id_type=MESH,
        )

    cross_copy = pltpu.make_async_remote_copy(
        pair.at[1 - zhalf], from_pair, x_send.at[0], x_recv.at[0],
        device_id=((((1 - zhalf) * nh + zin) * ny + y) * 2 + core, s), device_id_type=MESH,
    )

    def finish_planes():
        for copy in plane_copies:
            copy.wait()
        total = sum_core[:, y, s]
        for k in range(1, ny * ns):
            total = total + from_plane[k - 1]
        sum_plane[...] = total.reshape(2, nh, rows, 128)
        loop(1, nh, lambda k: line_copy(k).start())

    def cross_lines():
        loop(1, nh, lambda k: line_copy(k).wait())
        pair[...] = sum_plane[:, zin] + jnp.sum(from_line[...], axis=0)
        cross_copy.start()

    def gather_back(i):
        settle(gout.at[pl.ds(0, hb * na * backs[i][3]), :], g_recv.at[i])

    def returned(c, i):
        count = hb * na * rc
        high, low = split(
            jnp.concatenate(
                [
                    gout[pl.ds(c * count * zp + 2 * i + j, count, stride=zp), :]
                    for j in range(2)
                ],
                axis=1,
            )
        )
        return jnp.dot(
            table_i[half, c], jnp.concatenate([high, low, high], axis=0),
            preferred_element_type=jnp.float32,
        )

    def invert_chunk(c, i):
        value = returned(c, i)
        for j in range(2):
            here = value[:, j * width:(j + 1) * width]
            slopes[2 * i + j] = here if c == 0 else slopes[2 * i + j] + here

    rows_d = pl.ds(pl.multiple_of(half * hz, hz), hz)
    for m, (c, start, count) in enumerate(units):
        here = col.at[c, :, :, pl.ds(start * zp, count * zp), :]
        guard(whole, mine, functools.partial(settle, here, d_recv.at[m]))

        def derive_pair(j):
            k, r = lax.div(j, each), 2 * lax.rem(j, each)
            value = split(jnp.concatenate([column(c, k, r), column(c, k, r + 1)], axis=1))
            slope = dot3((table_d[0, rows_d, :], table_d[1, rows_d, :]), value)
            for i in range(2):
                spot = pl.ds(pl.multiple_of((r + i) * zp, zp), zl)
                grad[c, k, :, spot, :] = slope[:, i * width:(i + 1) * width].reshape(hb, zl, width)

        def derive_spins(j):
            r = start + j
            value = split(jnp.concatenate([column(c, k, r) for k in range(ns)], axis=1))
            slope = dot3((table_d[0, rows_d, :], table_d[1, rows_d, :]), value)
            for k in range(ns):
                spot = pl.ds(pl.multiple_of(r * zp, zp), zl)
                grad[c, k, :, spot, :] = slope[:, k * width:(k + 1) * width].reshape(hb, zl, width)

        def transform(i):
            j = c * each + i
            real, imag = column(c, 0, i), column(c, 0, each + i)
            for k in range(1, ns):
                real, imag = real + column(c, k, i), imag + column(c, k, each + i)
            position = jnp.full((nzg, width), place(j))
            imag = jnp.where(position % (nx // 2) == 0, 0.0, imag)
            value = split(jnp.concatenate([real, imag], axis=1))
            value = split(dot3(value, (table_y[0], table_y[1])))
            turned = dot3((table_z[0], table_z[1]), value)
            real = turned[:nzg, :width] + turned[nzg:, width:]
            imag = turned[:nzg, width:] - turned[nzg:, :width]
            inverse = inverses[j]
            here = s * per + j
            local = real * factor[0, :, here, :] + imag * factor[1, :, here, :]
            hartree = (4.0 * np.pi) * (real * real + imag * imag) * inverse
            weigh = 2.0 * (hartree * inverse + local)
            weigh_z = weigh * freq_z
            plain, along_z, along_zz = fold(weigh), fold(weigh_z), fold(weigh_z * freq_z)
            trace = fold(hartree)
            row_x = axis_frequency(position[:1], nx)
            terms = (
                plain * row_x * row_x - trace,
                plain * row_y * row_y - trace,
                along_zz - trace,
                along_z * row_y,
                along_z * row_x,
                plain * row_x * row_y,
            )
            for i, term in enumerate(terms):
                part[pl.ds(i, 1), :] += term

        def work():
            if count == rc:
                loop(0, ns * each, derive_pair)
            else:
                loop(0, count, derive_spins)
            for i in range(len(backs)):
                if backs[i][0] == m:
                    far_first(hb * ns, lambda k: back_copy(i, k).start())
                    local_back(i)

        def spectrum():
            loop(0, each, transform)

        guard(whole, mine, work)
        if m == max(chunks - 3, 0):
            finish_planes()
        send_stage(m + 2)
        if start + count == rc:
            guard(whole, mine, spectrum)
        if m == max(chunks - 2, 0):
            cross_lines()
        done = m - 2 if start else m - 1
        if 0 <= done and m != chunks - 1:
            gather_back(done)
            loop(0, zl // 2, functools.partial(invert_chunk, done))

    cross_copy.wait()
    kweight = pair[zhalf] + from_pair[...]
    fetches[9].wait()
    gk = [spacing * (miller[i].reshape(rows, 128).astype(jnp.float32) + kpoint[i]) for i in range(3)]
    kdens[...] = 0.5 * (gk[0] * gk[0] + gk[1] * gk[1] + gk[2] * gk[2]) * kweight
    scaled = kweight * (-1.0 / (n * rows * 128))
    order = ((0, 0), (1, 1), (2, 2), (1, 2), (0, 2), (0, 1))
    for i, (p, q) in enumerate(order):
        part[pl.ds(i, 1), :] += fold(scaled * gk[p] * gk[q])

    group = 2 if zl % 4 == 0 else 1

    def exchange(i):
        lasts = [returned(chunks - 1, group * i + m) for m in range(group)]
        tallies = [tally[t] for t in range(len(order))]
        for j in range(2 * group):
            spot = 2 * group * i + j
            here = lasts[j // 2][:, j % 2 * width:(j % 2 + 1) * width]
            if chunks > 1:
                here = here + slopes[spot]
            g = (grad_x[spot], grad_y[spot], here)
            total = g[0] * g[0] + g[1] * g[1] + g[2] * g[2]
            square[spot] = total
            value = dens[spot]
            weigh = above[spot] / (4.0 * value * value + 1.0 + total)
            scaled = [weigh * g[p] for p in range(3)]
            for t, (p, q) in enumerate(order):
                term = (scaled[p] * g[q]).reshape(nx // 8, 8, width)
                tallies[t] = tallies[t] + jnp.sum(term, axis=0)
        for t in range(len(order)):
            tally[t] = tallies[t]

    steps = zl // (2 * group)
    late = len(backs) - len(units)
    for i in range(chunks - 1, len(backs) - late):
        gather_back(i)
    loop(0, steps // (1 + late), exchange)
    if late:
        gather_back(len(backs) - 1)
        loop(steps // 2, steps, exchange)
    for t in range(len(order)):
        part[pl.ds(t, 1), :] += fold(tally[t])
    spots = [lax.broadcasted_iota(jnp.int32, (8, 128), i) for i in range(2)]
    sums = jnp.sum(part[...], axis=1, keepdims=True)
    row[...] = fold(jnp.where(spots[0] == spots[1], sums, 0.0))

    def stress_copy(k):
        return pltpu.make_async_remote_copy(
            row, held.at[k - 1], t_send.at[0], t_recv.at[0],
            device_id=partner(b, s, k, nb, ns), device_id_type=MESH,
        )

    def share_stress(k):
        stress_copy(k).start()

    def drain(c, count, semaphore):
        settle(out.at[0, pl.ds(0, count), :], semaphore.at[c])

    results = [
        pltpu.make_async_copy(value, target, o_sem.at[i])
        for i, (value, target) in enumerate(
            ((stress, stress_o), (kdens, kdens_o), (square, square_o))
        )
    ]
    far_first(n, share_stress)
    for result in results[1:]:
        result.start()
    for m, (_, _, count) in enumerate(units):
        guard(whole, mine, functools.partial(drain, m, (nb * na - 1) * count * zp, d_send))
        if not whole:
            pl.when(s >= na)(functools.partial(drain, m, nb * na * count * zp, d_send))
    for i in range(len(backs)):
        guard(whole, mine, functools.partial(drain, i, (hb * ns - 1) * backs[i][3], g_send))
    settle(held, t_send.at[0])
    settle(held, t_recv.at[0])
    stress[...] = row[...] + jnp.sum(held[...], axis=0)
    results[0].start()
    for result in results:
        result.wait()


def emit_kernel(stress, kdens, square, stress_o, kdens_o, square_o, semaphores):
    copies = [
        pltpu.make_async_copy(source, target, semaphores.at[i])
        for i, (source, target) in enumerate(((square, square_o), (kdens, kdens_o)))
    ]
    for copy in copies:
        copy.start()
    stress_o[...] = stress[0, :6]
    for copy in copies:
        copy.wait()


def params(number):
    return pltpu.CompilerParams(
        collective_id=number, has_side_effects=True, vmem_limit_bytes=60 * 2**20
    )


def vmem(*shape):
    return pltpu.VMEM(shape, jnp.float32)


def real_basis(nb, na, chunks, nx):
    xl = nx // nb
    per = xl // na
    each = per // chunks
    x = np.arange(nx)
    basis = np.zeros((chunks, nb, na, 2, each, nx))
    share = np.zeros((chunks, nb, na, 2, each))
    for b in range(nb):
        for j in range(xl):
            k = b * xl + j
            phases = (2.0 * np.pi / nx) * ((k * x) % nx)
            spot = (j % per // each, b, j // per, slice(None), j % each)
            if k % (nx // 2) == 0:
                other = (2.0 * np.pi / nx) * (((nx // 2 - k) * x) % nx)
                basis[spot] = np.stack([np.cos(phases), np.cos(other)])
                share[spot] = 1.0 / nx
            else:
                basis[spot] = np.stack([np.cos(phases), -np.sin(phases)])
                share[spot] = 2.0 / nx
    inverse = (basis * share[..., None]).reshape(chunks, 2, -1, nx)
    inverse = inverse.transpose(1, 0, 3, 2)
    return basis.reshape(chunks, -1, nx), inverse


def beside(table):
    return np.concatenate(list(host_split(table)), axis=-1)


def shards(nb, ns, coefficients, occupation, miller, density, local_factor):
    dma = pltpu.SemaphoreType.DMA
    _, zl, nx, ny = density.shape
    nzg = zl * nb
    xl = nx // nb
    na = min(ns, xl)
    per = xl // na
    chunks = min(CHUNKS, per)
    rc = 2 * (per // chunks)
    zp = zl
    while rc * zp % 8:
        zp += 1
    block = rc * zp
    npw = coefficients.shape[3]
    rows = npw // (nb * ns * 128)
    nbl = coefficients.shape[2]
    fold_y = 2 if nb % 4 == 0 else 1
    fold_z = nb // (2 * fold_y)
    hb = nb // 2

    coef = coefficients[0].reshape(2, nbl, npw // 128, 128)
    coef = coef.transpose(0, 2, 1, 3).reshape(2, npw // 128 * nbl, 128)
    basis, inverse = real_basis(nb, na, chunks, nx)
    cos_y, sin_y = fourier_tables(ny)
    cos_z, sin_z = fourier_tables(nzg)
    table_y = np.block([[cos_y, -sin_y], [sin_y, cos_y]])
    in_plane = [derivative_table(nx).astype(np.float64), derivative_table(ny).T.astype(np.float64)]
    fetched = (
        density[0],
        coef,
        local_factor,
        beside(basis),
        np.concatenate([host_split(inverse)[k] for k in (0, 0, 1)], axis=-1),
        host_split(table_y),
        host_split(derivative_table(nzg).astype(np.float64)),
        host_split(np.concatenate([cos_z, sin_z]) / (nzg * nx * ny)),
        host_split(np.stack(in_plane)),
        miller,
    )

    stress, kinetic_density, square = pl.pallas_call(
        functools.partial(main_kernel, nb, ns, fold_y, fold_z),
        out_shape=(vmem(1, 128), vmem(rows, 128), vmem(zl, nx, ny)),
        in_specs=[pl.BlockSpec(memory_space=pltpu.SMEM)]
        + [pl.BlockSpec(memory_space=pltpu.HBM)] * len(fetched),
        out_specs=(pl.BlockSpec(memory_space=pl.ANY),) * 3,
        scratch_shapes=[pltpu.VMEM(value.shape, value.dtype) for value in fetched]
        + [
            pltpu.VMEM(shape, jnp.float32)
            for shape in (
                (1, 128),
                (rows, 128),
                (zl, nx, ny),
                (2, rows * nbl, 128),
                (fold_z * fold_y, 2, ns, rows, 128),
                (chunks, nb * na * block, ny),
                (chunks, ns, nb, block, ny),
                (chunks, ns, hb, block, ny),
                (chunks * hb * na * block, ny),
                (fold_z * fold_y, ns, rows, 128),
                (fold_z, fold_y, ns, rows, 128),
                (fold_y * ns - 1, fold_z, rows, 128),
                (2, fold_z // 2, rows, 128),
                (fold_z // 2 - 1, 2, rows, 128),
                (2, rows, 128),
                (rows, 128),
                (per, nzg, ny),
                (zl, nx, ny),
                (zl, nx, ny),
                (zl, nx, ny),
                (zl, nx, ny),
                (6, 8, ny),
                (8, 128),
                (1, 128),
                (nb * ns - 1, 1, 128),
            )
        ]
        + [dma((len(fetched),)), dma((3,))]
        + [
            dma(shape)
            for shape in (
                (chunks + 1,), (1,), (fold_y * ns - 1,), (fold_z // 2 - 1,), (1,),
                (chunks + 2 if zl % 16 == 0 else chunks + 1,), (1,),
            )
            for _ in range(2)
        ],
        compiler_params=params(0),
        name="main_exchange",
    )(occupation, *fetched)
    anywhere = pl.BlockSpec(memory_space=pl.ANY)
    resident = pl.BlockSpec(memory_space=pltpu.VMEM)
    stress, kinetic_density, square = pl.pallas_call(
        emit_kernel,
        out_shape=[
            jax.ShapeDtypeStruct(shape, jnp.float32) for shape in ((6,), (rows, 128), (zl, nx, ny))
        ],
        in_specs=[resident, anywhere, anywhere],
        out_specs=[resident, anywhere, anywhere],
        scratch_shapes=[dma((2,))],
        compiler_params=pltpu.CompilerParams(vmem_limit_bytes=2**20),
        name="emit",
    )(stress, kinetic_density, square)
    return stress, kinetic_density.reshape(rows * 128), square[None]


def solution(mesh):
    return jax.shard_map(
        functools.partial(shards, mesh.shape["band"], mesh.shape["spin"]),
        mesh=mesh,
        in_specs=(
            P("spin", None, "band", None),
            P("spin", "band"),
            P(None, ("band", "spin")),
            P("spin", "band", None, None),
            P(None, None, "band", None),
        ),
        out_specs=(P(), P(("band", "spin")), P("spin", "band", None, None)),
        check_vma=False,
    )
```

```python
import functools

import jax
import jax.numpy as jnp
import numpy as np
from jax import lax
from jax.experimental import pallas as pl
from jax.experimental.pallas import tpu as pltpu
from jax.sharding import PartitionSpec as P

occupation_unit = 1000.0
kpoint = (0.25, 0.125, 0.375)
spacing = 0.25
MESH = pl.DeviceIdType.MESH
CHUNKS = 4
PLAN = (((0, 0), (1, 0)), ((0, 1), (0, 2), (0, 3), (0, 4), (1, 1), (1, 2)), (), ((1, 3), (1, 4)))


def derivative_table(length):
    index = np.arange(length)
    wrapped = np.mod(index[:, None] - index[None, :], length)
    angles = np.pi / length * wrapped
    sines = np.where(wrapped == 0, 1.0, np.sin(angles))
    parity = 1.0 - 2.0 * np.mod(wrapped, 2)
    table = np.where(wrapped == 0, 0.0, 0.5 * parity * np.cos(angles) / sines)
    return table.astype(np.float32)


def fourier_tables(length):
    index = np.arange(length)
    phases = np.mod(index[:, None] * index[None, :], length) * (2.0 * np.pi / length)
    return np.cos(phases), np.sin(phases)


def wrapped(value, count):
    return jnp.where(value >= count, value - count, value)


def far_first(count, step):
    loop(count // 2, count, step)
    loop(1, count // 2, step)


def spread(count, step):
    for k in (3, 1, 2, 0):
        loop(max(k * count // 4, 1), (k + 1) * count // 4, step)


def partner(b, s, offset, nb, ns):
    hop = lax.div(offset, ns)
    return wrapped(b + hop, nb), wrapped(s + offset - hop * ns, ns)


def greet_all(nb, ns):
    b, s = lax.axis_index("band"), lax.axis_index("spin")
    barrier = pltpu.get_barrier_semaphore()

    def greet(k):
        pl.semaphore_signal(
            barrier, inc=1, device_id=partner(b, s, k, nb, ns), device_id_type=MESH
        )

    spread(nb * ns, greet)
    return b, s


def split(value):
    high = value.astype(jnp.bfloat16)
    return high, (value - high.astype(jnp.float32)).astype(jnp.bfloat16)


def host_split(table):
    high = table.astype(np.float32).astype(jnp.bfloat16)
    low = (table - high.astype(np.float64)).astype(np.float32).astype(jnp.bfloat16)
    return np.stack([high, low])


def dot3(left, right):
    def one(p, q):
        return jnp.dot(p, q, preferred_element_type=jnp.float32)

    return one(left[0], right[0]) + (one(left[0], right[1]) + one(left[1], right[0]))


def loop(low, high, step):
    def body(k, carry):
        step(k)
        return carry

    lax.fori_loop(low, high, body, 0)


def axis_frequency(index, length):
    signed = jnp.where(index >= length // 2, index - length, index)
    return 2.0 * np.pi / length * signed.astype(jnp.float32)


def fold(value):
    return jnp.sum(value, axis=0, keepdims=True)


def guard(always, condition, step):
    if always:
        step()
    else:
        pl.when(condition)(step)


def stack3(left, right):
    high, low = right
    depth = high.shape[0]
    return jnp.dot(
        left, jnp.concatenate([high, high], axis=0), preferred_element_type=jnp.float32
    ) + jnp.dot(left[:, :depth], low, preferred_element_type=jnp.float32)


def settle(ref, semaphore):
    pltpu.make_async_copy(ref, ref, semaphore).wait()


def main_kernel(
    nb, ns, ny, nz, occupation_h, dens_h, coef_h, factor_h,
    table_f_h, table_i_h, table_y_h, table_d_h, table_z_h, table_g_h, miller_h,
    held, kdens_o, square_o,
    occupation, dens, coef, factor, table_f, table_i, table_y, table_d, table_z, table_g, miller,
    kdens, square, squares, kin, out, col, grad, gout, from_core, sum_core, from_plane, sum_plane, from_line, pair, from_pair,
    inverses, grad_x, grad_y, above, below, flat, slopes, tally, part, row,
    f_sem, o_sem, d_send, d_recv, c_send, c_recv, p_send, p_recv, l_send, l_recv, x_send, x_recv,
    g_send, g_recv, t_send, t_recv,
):
    sources = (dens_h, table_f_h, coef_h, table_g_h, table_d_h, table_y_h, table_z_h, factor_h, table_i_h, miller_h)
    targets = (dens, table_f, coef, table_g, table_d, table_y, table_z, factor, table_i, miller)
    fetches = [
        pltpu.make_async_copy(source, target, f_sem.at[i])
        for i, (source, target) in enumerate(zip(sources, targets))
    ]
    b, s = greet_all(nb, ns)
    for fetch in fetches[:2]:
        fetch.start()
    n = nb * ns
    core, y, z = b % 2, (b // 2) % ny, b // (2 * ny)
    zl, nx, width = dens.shape
    chunks, _, _, block, _ = col.shape
    hb = nb // 2
    half, u = b // hb, b % hb
    xl = nx // nb
    na = min(ns, xl)
    per = xl // na
    each = per // chunks
    rc = 2 * each
    zp = block // rc
    units = [(c, 0, rc) for c in range(chunks - 1)]
    units += [(chunks - 1, 0, each), (chunks - 1, each, each)]
    backs = [(m, c, r * zp, count * zp) for m, (c, r, count) in enumerate(units)]
    if zl % 16 == 0 and each == 1:
        m, c, edge, _ = backs.pop()
        backs += [(m, c, edge, zl // 2), (m, c, edge + zl // 2, zl // 2)]
    hz = hb * zl
    nzg = nb * zl
    rows = kdens.shape[0]
    whole, mine = na == ns, s < na
    for fetch in fetches[:2]:
        fetch.wait()
    fetches.append(pltpu.make_async_copy(occupation_h, occupation, f_sem.at[len(fetches)]))
    for fetch in fetches[2:]:
        fetch.start()

    def block_copy(m, k, cross):
        c, r, count = units[m]
        tu, ts = partner(u, s, k, hb, ns)
        tb = tu + hb * (1 - half if cross else half)
        at = pl.multiple_of((tb * na + ts) * block + r * zp, 8)
        return ts < na, pltpu.make_async_remote_copy(
            out.at[c, pl.ds(at, count * zp), :], col.at[c, s, b, pl.ds(r * zp, count * zp), :],
            d_send.at[m], d_recv.at[m], device_id=(tb, ts), device_id_type=MESH,
        )

    def forward(i, which):
        value = split(jnp.concatenate([dens[2 * i], dens[2 * i + 1]], axis=1))
        for c in which:
            turned = stack3(table_f[c], value)
            out[c, pl.ds(2 * i, nb * na * rc, stride=zp), :] = turned[:, :width]
            out[c, pl.ds(2 * i + 1, nb * na * rc, stride=zp), :] = turned[:, width:]

    def send_part(m, cross):
        def send(k):
            right, copy = block_copy(m, k, cross)
            guard(whole, right, copy.start)

        if cross:
            loop(0, hb * ns, send)
        else:
            far_first(hb * ns, send)

    def send_stage(stage):
        for cross, m in PLAN[stage] if stage < len(PLAN) else ():
            if m < len(units):
                send_part(m, cross)

    def keep(m):
        c, r, count = units[m]
        at = pl.multiple_of((b * na + s) * block + r * zp, 8)
        pltpu.make_async_copy(
            out.at[c, pl.ds(at, count * zp), :], col.at[c, s, b, pl.ds(r * zp, count * zp), :],
            d_recv.at[m],
        ).start()

    def forward_first(i):
        forward(i, range(1))

    def forward_rest(i):
        forward(i, range(1, chunks))

    loop(0, zl // 2, forward_first)
    pl.semaphore_wait(pltpu.get_barrier_semaphore(), n - 1)
    send_stage(0)

    fetches[2].wait()
    fetches[-1].wait()
    nbl = occupation.shape[1]
    depth = rows * nbl
    shares = [
        jnp.full((rows, 128), occupation[0, j]).astype(jnp.float32) / occupation_unit
        for j in range(nbl)
    ]
    def kinetic(i):
        for j in range(2):
            k = 2 * i + j
            here = pl.ds(pl.multiple_of(k * depth, depth), depth)
            real, imag = coef[0, here, :].astype(jnp.float32), coef[1, here, :].astype(jnp.float32)
            squares[j] = real * real + imag * imag
            total = shares[0] * squares[j, pl.ds(0, rows, stride=nbl), :]
            for m in range(1, nbl):
                total = total + shares[m] * squares[j, pl.ds(m, rows, stride=nbl), :]
            kin[lax.div(k, 2 * ns), lax.rem(lax.div(k, ns), 2), lax.rem(k, ns)] = total

    loop(0, n // 2, kinetic)
    core_copy = pltpu.make_async_remote_copy(
        kin.at[:, 1 - core], from_core, c_send.at[0], c_recv.at[0],
        device_id=(b + 1 - 2 * core, s), device_id_type=MESH,
    )
    core_copy.start()
    if chunks > 1:
        loop(0, zl // 2, forward_rest)
    core_copy.wait()

    def add_core(i):
        sum_core[lax.div(i, ny), lax.rem(i, ny)] = kin[i, core] + from_core[i]

    loop(0, nz * ny, add_core)
    plane_copies = []
    for k in range(1, ny * ns):
        ty, ts = (y + k // ns) % ny, (s + k % ns) % ns
        copy = pltpu.make_async_remote_copy(
            sum_core.at[:, ty, ts], from_plane.at[k - 1], p_send.at[k - 1], p_recv.at[k - 1],
            device_id=((z * ny + ty) * 2 + core, ts), device_id_type=MESH,
        )
        copy.start()
        plane_copies.append(copy)
    send_stage(1)
    for m in range(len(units)):
        guard(whole, mine, functools.partial(keep, m))

    fetches[3].wait()

    def in_plane(i):
        value = split(dens[i])
        slope_x = dot3((table_g[0, 0], table_g[1, 0]), value)
        slope_y = dot3(value, (table_g[0, 1], table_g[1, 1]))
        grad_x[i], grad_y[i] = slope_x, slope_y
        flat[i] = slope_x * slope_x + slope_y * slope_y
        scale = 4.0 * dens[i] * dens[i] + 1.0
        below[i] = scale + flat[i]
        weigh = jnp.exp(jnp.log(dens[i]) * (-1.0 / 3.0)) * scale
        above[i] = weigh * (-1.0 / (nzg * nx * width))

    loop(0, zl, in_plane)

    freq_z = axis_frequency(lax.broadcasted_iota(jnp.int32, (nzg, width), 0), nzg)
    freq_y = axis_frequency(lax.broadcasted_iota(jnp.int32, (nzg, width), 1), width)
    row_y = freq_y[:1]

    def place(j):
        return b * xl + s * per + j

    def invert(j):
        freq_x = axis_frequency(jnp.full((nzg, width), place(j)), nx)
        length = freq_x * freq_x + freq_y * freq_y + freq_z * freq_z
        positive = length > 0
        inverses[j] = jnp.where(positive, 1.0 / jnp.where(positive, length, 1.0), 0.0)

    loop(0, per, invert)

    part[...] = jnp.zeros_like(part)
    tally[...] = jnp.zeros_like(tally)
    for fetch in fetches[4:9]:
        fetch.wait()

    def back_copy(i, k):
        _, c, edge, count = backs[i]
        tu, ts = partner(u, s, k, hb, ns)
        at = pl.multiple_of(((c * hb + u) * na + s) * block + edge, 8)
        return pltpu.make_async_remote_copy(
            grad.at[c, ts, tu, pl.ds(edge, count), :], gout.at[pl.ds(at, count), :],
            g_send.at[i], g_recv.at[i], device_id=(half * hb + tu, ts), device_id_type=MESH,
        )

    def local_back(i):
        _, c, edge, count = backs[i]
        at = pl.multiple_of(((c * hb + u) * na + s) * block + edge, 8)
        pltpu.make_async_copy(
            grad.at[c, s, u, pl.ds(edge, count), :], gout.at[pl.ds(at, count), :], g_recv.at[i]
        ).start()

    def column(c, k, r):
        return col[c, k, :, pl.ds(pl.multiple_of(r * zp, zp), zl), :].reshape(nzg, width)

    nh = nz // 2
    zhalf, zin = z // nh, z % nh

    def line_copy(k):
        tz = (zin + k) % nh
        return pltpu.make_async_remote_copy(
            sum_plane.at[:, tz], from_line.at[k - 1], l_send.at[k - 1], l_recv.at[k - 1],
            device_id=(((zhalf * nh + tz) * ny + y) * 2 + core, s), device_id_type=MESH,
        )

    cross_copy = pltpu.make_async_remote_copy(
        pair.at[1 - zhalf], from_pair, x_send.at[0], x_recv.at[0],
        device_id=((((1 - zhalf) * nh + zin) * ny + y) * 2 + core, s), device_id_type=MESH,
    )

    def finish_planes():
        for copy in plane_copies:
            copy.wait()
        total = sum_core[:, y, s]
        for k in range(1, ny * ns):
            total = total + from_plane[k - 1]
        sum_plane[...] = total.reshape(2, nh, rows, 128)
        loop(1, nh, lambda k: line_copy(k).start())

    def cross_lines():
        loop(1, nh, lambda k: line_copy(k).wait())
        pair[...] = sum_plane[:, zin] + jnp.sum(from_line[...], axis=0)
        cross_copy.start()

    def gather_back(i):
        settle(gout.at[pl.ds(0, hb * na * backs[i][3]), :], g_recv.at[i])

    def returned(c, i):
        count = hb * na * rc
        high, low = split(
            jnp.concatenate(
                [
                    gout[pl.ds(c * count * zp + 2 * i + j, count, stride=zp), :]
                    for j in range(2)
                ],
                axis=1,
            )
        )
        return jnp.dot(
            table_i[half, c], jnp.concatenate([high, low, high], axis=0),
            preferred_element_type=jnp.float32,
        )

    def invert_chunk(c, i):
        value = returned(c, i)
        for j in range(2):
            here = value[:, j * width:(j + 1) * width]
            slopes[2 * i + j] = here if c == 0 else slopes[2 * i + j] + here

    rows_d = pl.ds(pl.multiple_of(half * hz, hz), hz)
    for m, (c, start, count) in enumerate(units):
        here = col.at[c, :, :, pl.ds(start * zp, count * zp), :]
        guard(whole, mine, functools.partial(settle, here, d_recv.at[m]))

        def derive_pair(j):
            k, r = lax.div(j, each), 2 * lax.rem(j, each)
            value = split(jnp.concatenate([column(c, k, r), column(c, k, r + 1)], axis=1))
            slope = dot3((table_d[0, rows_d, :], table_d[1, rows_d, :]), value)
            for i in range(2):
                spot = pl.ds(pl.multiple_of((r + i) * zp, zp), zl)
                grad[c, k, :, spot, :] = slope[:, i * width:(i + 1) * width].reshape(hb, zl, width)

        def derive_spins(j):
            r = start + j
            value = split(jnp.concatenate([column(c, k, r) for k in range(ns)], axis=1))
            slope = dot3((table_d[0, rows_d, :], table_d[1, rows_d, :]), value)
            for k in range(ns):
                spot = pl.ds(pl.multiple_of(r * zp, zp), zl)
                grad[c, k, :, spot, :] = slope[:, k * width:(k + 1) * width].reshape(hb, zl, width)

        def transform(i):
            j = c * each + i
            real, imag = column(c, 0, i), column(c, 0, each + i)
            for k in range(1, ns):
                real, imag = real + column(c, k, i), imag + column(c, k, each + i)
            position = jnp.full((nzg, width), place(j))
            imag = jnp.where(position % (nx // 2) == 0, 0.0, imag)
            value = split(jnp.concatenate([real, imag], axis=1))
            value = split(dot3(value, (table_y[0], table_y[1])))
            turned = dot3((table_z[0], table_z[1]), value)
            real = turned[:nzg, :width] + turned[nzg:, width:]
            imag = turned[:nzg, width:] - turned[nzg:, :width]
            inverse = inverses[j]
            here = s * per + j
            local = real * factor[0, :, here, :] + imag * factor[1, :, here, :]
            hartree = (4.0 * np.pi) * (real * real + imag * imag) * inverse
            weigh = 2.0 * (hartree * inverse + local)
            weigh_z = weigh * freq_z
            plain, along_z, along_zz = fold(weigh), fold(weigh_z), fold(weigh_z * freq_z)
            trace = fold(hartree)
            row_x = axis_frequency(position[:1], nx)
            terms = (
                plain * row_x * row_x - trace,
                plain * row_y * row_y - trace,
                along_zz - trace,
                along_z * row_y,
                along_z * row_x,
                plain * row_x * row_y,
            )
            for i, term in enumerate(terms):
                part[pl.ds(i, 1), :] += term

        def work():
            if count == rc:
                loop(0, ns * each, derive_pair)
            else:
                loop(0, count, derive_spins)
            for i in range(len(backs)):
                if backs[i][0] == m:
                    far_first(hb * ns, lambda k: back_copy(i, k).start())
                    local_back(i)

        def spectrum():
            loop(0, each, transform)

        guard(whole, mine, work)
        if m == max(chunks - 3, 0):
            finish_planes()
        send_stage(m + 2)
        if start + count == rc:
            guard(whole, mine, spectrum)
        if m == max(chunks - 2, 0):
            cross_lines()
        done = m - 2 if start else m - 1
        if 0 <= done and m != chunks - 1:
            gather_back(done)
            loop(0, zl // 2, functools.partial(invert_chunk, done))

    cross_copy.wait()
    kweight = pair[zhalf] + from_pair[...]
    fetches[9].wait()
    gk = [spacing * (miller[i].reshape(rows, 128).astype(jnp.float32) + kpoint[i]) for i in range(3)]
    kdens[...] = 0.5 * (gk[0] * gk[0] + gk[1] * gk[1] + gk[2] * gk[2]) * kweight
    scaled = kweight * (-1.0 / (n * rows * 128))
    order = ((0, 0), (1, 1), (2, 2), (1, 2), (0, 2), (0, 1))
    for i, (p, q) in enumerate(order):
        part[pl.ds(i, 1), :] += fold(scaled * gk[p] * gk[q])

    group = 2 if zl % 4 == 0 else 1

    def exchange(i):
        lasts = [returned(chunks - 1, group * i + m) for m in range(group)]
        tallies = [tally[t] for t in range(len(order))]
        for j in range(2 * group):
            spot = 2 * group * i + j
            here = lasts[j // 2][:, j % 2 * width:(j % 2 + 1) * width]
            if chunks > 1:
                here = here + slopes[spot]
            g = (grad_x[spot], grad_y[spot], here)
            rise = here * here
            square[spot] = flat[spot] + rise
            weigh = above[spot] / (below[spot] + rise)
            scaled = [weigh * g[p] for p in range(3)]
            for t, (p, q) in enumerate(order):
                term = (scaled[p] * g[q]).reshape(nx // 8, 8, width)
                tallies[t] = tallies[t] + jnp.sum(term, axis=0)
        for t in range(len(order)):
            tally[t] = tallies[t]

    steps = zl // (2 * group)
    late = len(backs) - len(units)
    for i in range(chunks - 1, len(backs) - late):
        gather_back(i)
    loop(0, steps // (1 + late), exchange)
    if late:
        gather_back(len(backs) - 1)
        loop(steps // 2, steps, exchange)
    for t in range(len(order)):
        part[pl.ds(t, 1), :] += fold(tally[t])
    spots = [lax.broadcasted_iota(jnp.int32, (8, 128), i) for i in range(2)]
    sums = jnp.sum(part[...], axis=1, keepdims=True)
    row[...] = fold(jnp.where(spots[0] == spots[1], sums, 0.0))

    def stress_copy(k):
        return pltpu.make_async_remote_copy(
            row, held.at[k - 1], t_send.at[0], t_recv.at[0],
            device_id=partner(b, s, k, nb, ns), device_id_type=MESH,
        )

    def share_stress(k):
        stress_copy(k).start()

    def drain(c, count, semaphore):
        settle(out.at[0, pl.ds(0, count), :], semaphore.at[c])

    results = [
        pltpu.make_async_copy(value, target, o_sem.at[i])
        for i, (value, target) in enumerate(
            ((kdens, kdens_o), (square, square_o))
        )
    ]
    spread(n, share_stress)
    pltpu.make_async_copy(row, held.at[n - 1], t_recv.at[0]).start()
    for result in results:
        result.start()
    for m, (_, _, count) in enumerate(units):
        guard(whole, mine, functools.partial(drain, m, (nb * na - 1) * count * zp, d_send))
        if not whole:
            pl.when(s >= na)(functools.partial(drain, m, nb * na * count * zp, d_send))
    for i in range(len(backs)):
        guard(whole, mine, functools.partial(drain, i, (hb * ns - 1) * backs[i][3], g_send))
    settle(held.at[pl.ds(0, n - 1)], t_send.at[0])
    for result in results:
        result.wait()
    settle(held, t_recv.at[0])


def emit_kernel(held, kdens, square, stress_o, kdens_o, square_o, semaphores):
    step = max(square.shape[0] // 4, 1)
    pieces = [
        (square.at[pl.ds(i, step)], square_o.at[pl.ds(i, step)])
        for i in range(0, square.shape[0], step)
    ]
    pieces.append((kdens, kdens_o))
    copies = [
        pltpu.make_async_copy(source, target, semaphores.at[i])
        for i, (source, target) in enumerate(pieces)
    ]
    for copy in copies:
        copy.start()
    stress_o[...] = jnp.sum(held[...], axis=0)[0, :6]
    for copy in copies:
        copy.wait()


def params(number):
    return pltpu.CompilerParams(
        collective_id=number, has_side_effects=True, vmem_limit_bytes=60 * 2**20
    )


def vmem(*shape):
    return pltpu.VMEM(shape, jnp.float32)


def real_basis(nb, na, chunks, nx):
    xl = nx // nb
    per = xl // na
    each = per // chunks
    x = np.arange(nx)
    basis = np.zeros((chunks, nb, na, 2, each, nx))
    share = np.zeros((chunks, nb, na, 2, each))
    for b in range(nb):
        for j in range(xl):
            k = b * xl + j
            phases = (2.0 * np.pi / nx) * ((k * x) % nx)
            spot = (j % per // each, b, j // per, slice(None), j % each)
            if k % (nx // 2) == 0:
                other = (2.0 * np.pi / nx) * (((nx // 2 - k) * x) % nx)
                basis[spot] = np.stack([np.cos(phases), np.cos(other)])
                share[spot] = 1.0 / nx
            else:
                basis[spot] = np.stack([np.cos(phases), -np.sin(phases)])
                share[spot] = 2.0 / nx
    inverse = (basis * share[..., None]).reshape(chunks, 2, -1, nx)
    inverse = inverse.transpose(1, 0, 3, 2)
    return basis.reshape(chunks, -1, nx), inverse


def beside(table):
    return np.concatenate(list(host_split(table)), axis=-1)


def shards(nb, ns, coefficients, occupation, miller, density, local_factor):
    dma = pltpu.SemaphoreType.DMA
    _, zl, nx, ny = density.shape
    nzg = zl * nb
    xl = nx // nb
    na = min(ns, xl)
    per = xl // na
    chunks = min(CHUNKS, per)
    rc = 2 * (per // chunks)
    zp = zl
    while rc * zp % 8:
        zp += 1
    block = rc * zp
    npw = coefficients.shape[3]
    rows = npw // (nb * ns * 128)
    nbl = coefficients.shape[2]
    fold_y = 2 if nb % 4 == 0 else 1
    fold_z = nb // (2 * fold_y)
    hb = nb // 2

    coef = coefficients[0].reshape(2, nbl, npw // 128, 128)
    coef = coef.transpose(0, 2, 1, 3).reshape(2, npw // 128 * nbl, 128)
    basis, inverse = real_basis(nb, na, chunks, nx)
    cos_y, sin_y = fourier_tables(ny)
    cos_z, sin_z = fourier_tables(nzg)
    table_y = np.block([[cos_y, -sin_y], [sin_y, cos_y]])
    in_plane = [derivative_table(nx).astype(np.float64), derivative_table(ny).T.astype(np.float64)]
    fetched = (
        density[0],
        coef,
        local_factor,
        beside(basis),
        np.concatenate([host_split(inverse)[k] for k in (0, 0, 1)], axis=-1),
        host_split(table_y),
        host_split(derivative_table(nzg).astype(np.float64)),
        host_split(np.concatenate([cos_z, sin_z]) / (nzg * nx * ny)),
        host_split(np.stack(in_plane)),
        miller,
    )

    held, kinetic_density, square = pl.pallas_call(
        functools.partial(main_kernel, nb, ns, fold_y, fold_z),
        out_shape=(vmem(nb * ns, 1, 128), vmem(rows, 128), vmem(zl, nx, ny)),
        in_specs=[pl.BlockSpec(memory_space=pltpu.HBM)] * (len(fetched) + 1),
        out_specs=(pl.BlockSpec(memory_space=pl.ANY),) * 3,
        scratch_shapes=[pltpu.SMEM(occupation.shape, occupation.dtype)]
        + [pltpu.VMEM(value.shape, value.dtype) for value in fetched]
        + [
            pltpu.VMEM(shape, jnp.float32)
            for shape in (
                (rows, 128),
                (zl, nx, ny),
                (2, rows * nbl, 128),
                (fold_z * fold_y, 2, ns, rows, 128),
                (chunks, nb * na * block, ny),
                (chunks, ns, nb, block, ny),
                (chunks, ns, hb, block, ny),
                (chunks * hb * na * block, ny),
                (fold_z * fold_y, ns, rows, 128),
                (fold_z, fold_y, ns, rows, 128),
                (fold_y * ns - 1, fold_z, rows, 128),
                (2, fold_z // 2, rows, 128),
                (fold_z // 2 - 1, 2, rows, 128),
                (2, rows, 128),
                (rows, 128),
                (per, nzg, ny),
                (zl, nx, ny),
                (zl, nx, ny),
                (zl, nx, ny),
                (zl, nx, ny),
                (zl, nx, ny),
                (zl, nx, ny),
                (6, 8, ny),
                (8, 128),
                (1, 128),
            )
        ]
        + [dma((len(fetched) + 1,)), dma((2,))]
        + [
            dma(shape)
            for shape in (
                (chunks + 1,), (1,), (fold_y * ns - 1,), (fold_z // 2 - 1,), (1,),
                (chunks + 2 if zl % 16 == 0 else chunks + 1,), (1,),
            )
            for _ in range(2)
        ],
        compiler_params=params(0),
        name="main_exchange",
    )(occupation, *fetched)
    anywhere = pl.BlockSpec(memory_space=pl.ANY)
    resident = pl.BlockSpec(memory_space=pltpu.VMEM)
    stress, kinetic_density, square = pl.pallas_call(
        emit_kernel,
        out_shape=[
            jax.ShapeDtypeStruct(shape, jnp.float32) for shape in ((6,), (rows, 128), (zl, nx, ny))
        ],
        in_specs=[resident, anywhere, anywhere],
        out_specs=[resident, anywhere, anywhere],
        scratch_shapes=[dma((5,))],
        compiler_params=pltpu.CompilerParams(vmem_limit_bytes=2**20),
        name="emit",
    )(held, kinetic_density, square)
    return stress, kinetic_density.reshape(rows * 128), square[None]


def solution(mesh):
    return jax.shard_map(
        functools.partial(shards, mesh.shape["band"], mesh.shape["spin"]),
        mesh=mesh,
        in_specs=(
            P("spin", None, "band", None),
            P("spin", "band"),
            P(None, ("band", "spin")),
            P("spin", "band", None, None),
            P(None, None, "band", None),
        ),
        out_specs=(P(), P(("band", "spin")), P("spin", "band", None, None)),
        check_vma=False,
    )
```

```python
import functools

import jax
import jax.numpy as jnp
import numpy as np
from jax import lax
from jax.experimental import pallas as pl
from jax.experimental.pallas import tpu as pltpu
from jax.sharding import PartitionSpec as P

occupation_unit = 1000.0
kpoint = (0.25, 0.125, 0.375)
spacing = 0.25
MESH = pl.DeviceIdType.MESH
CHUNKS = 4
PLAN = (((0, 0), (1, 0)), ((0, 1), (0, 2), (0, 3), (0, 4), (1, 1), (1, 2)), (), ((1, 3), (1, 4)))


def derivative_table(length):
    index = np.arange(length)
    wrapped = np.mod(index[:, None] - index[None, :], length)
    angles = np.pi / length * wrapped
    sines = np.where(wrapped == 0, 1.0, np.sin(angles))
    parity = 1.0 - 2.0 * np.mod(wrapped, 2)
    table = np.where(wrapped == 0, 0.0, 0.5 * parity * np.cos(angles) / sines)
    return table.astype(np.float32)


def fourier_tables(length):
    index = np.arange(length)
    phases = np.mod(index[:, None] * index[None, :], length) * (2.0 * np.pi / length)
    return np.cos(phases), np.sin(phases)


def wrapped(value, count):
    return jnp.where(value >= count, value - count, value)


def far_first(count, step):
    loop(count // 2, count, step)
    loop(1, count // 2, step)


def spread(count, step):
    for k in (3, 1, 2, 0):
        loop(max(k * count // 4, 1), (k + 1) * count // 4, step)


def partner(b, s, offset, nb, ns):
    hop = lax.div(offset, ns)
    return wrapped(b + hop, nb), wrapped(s + offset - hop * ns, ns)


def greet_all(nb, ns):
    b, s = lax.axis_index("band"), lax.axis_index("spin")
    barrier = pltpu.get_barrier_semaphore()

    def greet(k):
        pl.semaphore_signal(
            barrier, inc=1, device_id=partner(b, s, k, nb, ns), device_id_type=MESH
        )

    spread(nb * ns, greet)
    return b, s


def split(value):
    high = value.astype(jnp.bfloat16)
    return high, (value - high.astype(jnp.float32)).astype(jnp.bfloat16)


def host_split(table):
    high = table.astype(np.float32).astype(jnp.bfloat16)
    low = (table - high.astype(np.float64)).astype(np.float32).astype(jnp.bfloat16)
    return np.stack([high, low])


def dot3(left, right):
    def one(p, q):
        return jnp.dot(p, q, preferred_element_type=jnp.float32)

    return one(left[0], right[0]) + (one(left[0], right[1]) + one(left[1], right[0]))


def loop(low, high, step):
    def body(k, carry):
        step(k)
        return carry

    lax.fori_loop(low, high, body, 0)


def axis_frequency(index, length):
    signed = jnp.where(index >= length // 2, index - length, index)
    return 2.0 * np.pi / length * signed.astype(jnp.float32)


def fold(value):
    return jnp.sum(value, axis=0, keepdims=True)


def guard(always, condition, step):
    if always:
        step()
    else:
        pl.when(condition)(step)


def stack3(left, right):
    high, low = right
    depth = high.shape[0]
    return jnp.dot(
        left, jnp.concatenate([high, high], axis=0), preferred_element_type=jnp.float32
    ) + jnp.dot(left[:, :depth], low, preferred_element_type=jnp.float32)


def settle(ref, semaphore):
    pltpu.make_async_copy(ref, ref, semaphore).wait()


def main_kernel(
    nb, ns, ny, nz, occupation_h, dens_h, coef_h, factor_h,
    table_f_h, table_i_h, table_y_h, table_d_h, table_z_h, table_g_h, miller_h,
    held, kdens_o, square_o,
    occupation, dens, coef, factor, table_f, table_i, table_y, table_d, table_z, table_g, miller,
    kdens, square, squares, kin, out, col, grad, gout, from_core, sum_core, from_plane, sum_plane, from_line, pair, from_pair,
    inverses, grad_x, grad_y, above, below, flat, slopes, tally, part, row,
    f_sem, o_sem, d_send, d_recv, c_send, c_recv, p_send, p_recv, l_send, l_recv, x_send, x_recv,
    g_send, g_recv, t_send, t_recv,
):
    sources = (dens_h, table_f_h, coef_h, table_g_h, table_d_h, table_y_h, table_z_h, factor_h, table_i_h, miller_h)
    targets = (dens, table_f, coef, table_g, table_d, table_y, table_z, factor, table_i, miller)
    fetches = [
        pltpu.make_async_copy(source, target, f_sem.at[i])
        for i, (source, target) in enumerate(zip(sources, targets))
    ]
    b, s = greet_all(nb, ns)
    for fetch in fetches[:2]:
        fetch.start()
    n = nb * ns
    core, y, z = b % 2, (b // 2) % ny, b // (2 * ny)
    zl, nx, width = dens.shape
    chunks, _, _, block, _ = col.shape
    hb = nb // 2
    half, u = b // hb, b % hb
    xl = nx // nb
    na = min(ns, xl)
    per = xl // na
    each = per // chunks
    rc = 2 * each
    zp = block // rc
    units = [(c, 0, rc) for c in range(chunks - 1)]
    units += [(chunks - 1, 0, each), (chunks - 1, each, each)]
    backs = [(m, c, r * zp, count * zp) for m, (c, r, count) in enumerate(units)]
    if zl % 16 == 0 and each == 1:
        m, c, edge, _ = backs.pop()
        backs += [(m, c, edge, zl // 2), (m, c, edge + zl // 2, zl // 2)]
    hz = hb * zl
    nzg = nb * zl
    rows = kdens.shape[0]
    whole, mine = na == ns, s < na
    for fetch in fetches[:2]:
        fetch.wait()
    fetches.append(pltpu.make_async_copy(occupation_h, occupation, f_sem.at[len(fetches)]))
    for fetch in fetches[2:]:
        fetch.start()

    def block_copy(m, k, cross):
        c, r, count = units[m]
        tu, ts = partner(u, s, k, hb, ns)
        tb = tu + hb * (1 - half if cross else half)
        at = pl.multiple_of((tb * na + ts) * block + r * zp, 8)
        return ts < na, pltpu.make_async_remote_copy(
            out.at[c, pl.ds(at, count * zp), :], col.at[c, s, b, pl.ds(r * zp, count * zp), :],
            d_send.at[0], d_recv.at[m], device_id=(tb, ts), device_id_type=MESH,
        )

    def forward(i, which):
        value = split(jnp.concatenate([dens[2 * i], dens[2 * i + 1]], axis=1))
        for c in which:
            turned = stack3(table_f[c], value)
            out[c, pl.ds(2 * i, nb * na * rc, stride=zp), :] = turned[:, :width]
            out[c, pl.ds(2 * i + 1, nb * na * rc, stride=zp), :] = turned[:, width:]

    def send_part(m, cross):
        def send(k):
            right, copy = block_copy(m, k, cross)
            guard(whole, right, copy.start)

        if cross:
            loop(0, hb * ns, send)
        else:
            far_first(hb * ns, send)

    def send_stage(stage):
        for cross, m in PLAN[stage] if stage < len(PLAN) else ():
            if m < len(units):
                send_part(m, cross)

    def keep(m):
        c, r, count = units[m]
        at = pl.multiple_of((b * na + s) * block + r * zp, 8)
        pltpu.make_async_copy(
            out.at[c, pl.ds(at, count * zp), :], col.at[c, s, b, pl.ds(r * zp, count * zp), :],
            d_recv.at[m],
        ).start()

    def forward_first(i):
        forward(i, range(1))

    def forward_rest(i):
        forward(i, range(1, chunks))

    loop(0, zl // 2, forward_first)
    pl.semaphore_wait(pltpu.get_barrier_semaphore(), n - 1)
    send_stage(0)

    fetches[2].wait()
    fetches[-1].wait()
    nbl = occupation.shape[1]
    depth = rows * nbl
    shares = [
        jnp.full((rows, 128), occupation[0, j]).astype(jnp.float32) / occupation_unit
        for j in range(nbl)
    ]
    def kinetic(i):
        for j in range(2):
            k = 2 * i + j
            here = pl.ds(pl.multiple_of(k * depth, depth), depth)
            real, imag = coef[0, here, :].astype(jnp.float32), coef[1, here, :].astype(jnp.float32)
            squares[j] = real * real + imag * imag
            total = shares[0] * squares[j, pl.ds(0, rows, stride=nbl), :]
            for m in range(1, nbl):
                total = total + shares[m] * squares[j, pl.ds(m, rows, stride=nbl), :]
            kin[lax.div(k, 2 * ns), lax.rem(lax.div(k, ns), 2), lax.rem(k, ns)] = total

    loop(0, n // 2, kinetic)
    core_copy = pltpu.make_async_remote_copy(
        kin.at[:, 1 - core], from_core, c_send.at[0], c_recv.at[0],
        device_id=(b + 1 - 2 * core, s), device_id_type=MESH,
    )
    core_copy.start()
    if chunks > 1:
        loop(0, zl // 2, forward_rest)
    core_copy.wait()

    def add_core(i):
        sum_core[lax.div(i, ny), lax.rem(i, ny)] = kin[i, core] + from_core[i]

    loop(0, nz * ny, add_core)
    plane_copies = []
    for k in range(1, ny * ns):
        ty, ts = (y + k // ns) % ny, (s + k % ns) % ns
        copy = pltpu.make_async_remote_copy(
            sum_core.at[:, ty, ts], from_plane.at[k - 1], p_send.at[k - 1], p_recv.at[k - 1],
            device_id=((z * ny + ty) * 2 + core, ts), device_id_type=MESH,
        )
        copy.start()
        plane_copies.append(copy)
    send_stage(1)
    for m in range(len(units)):
        guard(whole, mine, functools.partial(keep, m))

    fetches[3].wait()

    def in_plane(i):
        value = split(dens[i])
        slope_x = dot3((table_g[0, 0], table_g[1, 0]), value)
        slope_y = dot3(value, (table_g[0, 1], table_g[1, 1]))
        grad_x[i], grad_y[i] = slope_x, slope_y
        flat[i] = slope_x * slope_x + slope_y * slope_y
        scale = 4.0 * dens[i] * dens[i] + 1.0
        below[i] = scale + flat[i]
        weigh = jnp.exp(jnp.log(dens[i]) * (-1.0 / 3.0)) * scale
        above[i] = weigh * (-1.0 / (nzg * nx * width))

    loop(0, zl, in_plane)

    freq_z = axis_frequency(lax.broadcasted_iota(jnp.int32, (nzg, width), 0), nzg)
    freq_y = axis_frequency(lax.broadcasted_iota(jnp.int32, (nzg, width), 1), width)
    row_y = freq_y[:1]

    def place(j):
        return b * xl + s * per + j

    def invert(j):
        freq_x = axis_frequency(jnp.full((nzg, width), place(j)), nx)
        length = freq_x * freq_x + freq_y * freq_y + freq_z * freq_z
        positive = length > 0
        inverses[j] = jnp.where(positive, 1.0 / jnp.where(positive, length, 1.0), 0.0)

    loop(0, per, invert)

    part[...] = jnp.zeros_like(part)
    tally[...] = jnp.zeros_like(tally)
    for fetch in fetches[4:9]:
        fetch.wait()

    def back_copy(i, k):
        _, c, edge, count = backs[i]
        tu, ts = partner(u, s, k, hb, ns)
        at = pl.multiple_of(((c * hb + u) * na + s) * block + edge, 8)
        return pltpu.make_async_remote_copy(
            grad.at[c, ts, tu, pl.ds(edge, count), :], gout.at[pl.ds(at, count), :],
            g_send.at[0], g_recv.at[i], device_id=(half * hb + tu, ts), device_id_type=MESH,
        )

    def local_back(i):
        _, c, edge, count = backs[i]
        at = pl.multiple_of(((c * hb + u) * na + s) * block + edge, 8)
        pltpu.make_async_copy(
            grad.at[c, s, u, pl.ds(edge, count), :], gout.at[pl.ds(at, count), :], g_recv.at[i]
        ).start()

    def column(c, k, r):
        return col[c, k, :, pl.ds(pl.multiple_of(r * zp, zp), zl), :].reshape(nzg, width)

    nh = nz // 2
    zhalf, zin = z // nh, z % nh

    def line_copy(k):
        tz = (zin + k) % nh
        return pltpu.make_async_remote_copy(
            sum_plane.at[:, tz], from_line.at[k - 1], l_send.at[k - 1], l_recv.at[k - 1],
            device_id=(((zhalf * nh + tz) * ny + y) * 2 + core, s), device_id_type=MESH,
        )

    cross_copy = pltpu.make_async_remote_copy(
        pair.at[1 - zhalf], from_pair, x_send.at[0], x_recv.at[0],
        device_id=((((1 - zhalf) * nh + zin) * ny + y) * 2 + core, s), device_id_type=MESH,
    )

    def finish_planes():
        for copy in plane_copies:
            copy.wait()
        total = sum_core[:, y, s]
        for k in range(1, ny * ns):
            total = total + from_plane[k - 1]
        sum_plane[...] = total.reshape(2, nh, rows, 128)
        loop(1, nh, lambda k: line_copy(k).start())

    def cross_lines():
        loop(1, nh, lambda k: line_copy(k).wait())
        pair[...] = sum_plane[:, zin] + jnp.sum(from_line[...], axis=0)
        cross_copy.start()

    def gather_back(i):
        settle(gout.at[pl.ds(0, hb * na * backs[i][3]), :], g_recv.at[i])

    def returned(c, i):
        count = hb * na * rc
        high, low = split(
            jnp.concatenate(
                [
                    gout[pl.ds(c * count * zp + 2 * i + j, count, stride=zp), :]
                    for j in range(2)
                ],
                axis=1,
            )
        )
        return jnp.dot(
            table_i[half, c], jnp.concatenate([high, low, high], axis=0),
            preferred_element_type=jnp.float32,
        )

    def invert_chunk(c, i):
        value = returned(c, i)
        for j in range(2):
            here = value[:, j * width:(j + 1) * width]
            slopes[2 * i + j] = here if c == 0 else slopes[2 * i + j] + here

    rows_d = pl.ds(pl.multiple_of(half * hz, hz), hz)
    for m, (c, start, count) in enumerate(units):
        here = col.at[c, :, :, pl.ds(start * zp, count * zp), :]
        guard(whole, mine, functools.partial(settle, here, d_recv.at[m]))

        def derive_pair(j):
            k, r = lax.div(j, each), 2 * lax.rem(j, each)
            value = split(jnp.concatenate([column(c, k, r), column(c, k, r + 1)], axis=1))
            slope = dot3((table_d[0, rows_d, :], table_d[1, rows_d, :]), value)
            for i in range(2):
                spot = pl.ds(pl.multiple_of((r + i) * zp, zp), zl)
                grad[c, k, :, spot, :] = slope[:, i * width:(i + 1) * width].reshape(hb, zl, width)

        def derive_spins(j):
            r = start + j
            value = split(jnp.concatenate([column(c, k, r) for k in range(ns)], axis=1))
            slope = dot3((table_d[0, rows_d, :], table_d[1, rows_d, :]), value)
            for k in range(ns):
                spot = pl.ds(pl.multiple_of(r * zp, zp), zl)
                grad[c, k, :, spot, :] = slope[:, k * width:(k + 1) * width].reshape(hb, zl, width)

        def transform(c, i):
            j = c * each + i
            real, imag = column(c, 0, i), column(c, 0, each + i)
            for k in range(1, ns):
                real, imag = real + column(c, k, i), imag + column(c, k, each + i)
            position = jnp.full((nzg, width), place(j))
            imag = jnp.where(position % (nx // 2) == 0, 0.0, imag)
            value = split(jnp.concatenate([real, imag], axis=1))
            value = split(dot3(value, (table_y[0], table_y[1])))
            turned = dot3((table_z[0], table_z[1]), value)
            real = turned[:nzg, :width] + turned[nzg:, width:]
            imag = turned[:nzg, width:] - turned[nzg:, :width]
            inverse = inverses[j]
            here = s * per + j
            local = real * factor[0, :, here, :] + imag * factor[1, :, here, :]
            hartree = (4.0 * np.pi) * (real * real + imag * imag) * inverse
            weigh = 2.0 * (hartree * inverse + local)
            weigh_z = weigh * freq_z
            plain, along_z, along_zz = fold(weigh), fold(weigh_z), fold(weigh_z * freq_z)
            trace = fold(hartree)
            row_x = axis_frequency(position[:1], nx)
            terms = (
                plain * row_x * row_x - trace,
                plain * row_y * row_y - trace,
                along_zz - trace,
                along_z * row_y,
                along_z * row_x,
                plain * row_x * row_y,
            )
            for i, term in enumerate(terms):
                part[pl.ds(i, 1), :] += term

        def work():
            if count == rc:
                loop(0, ns * each, derive_pair)
            else:
                loop(0, count, derive_spins)
            for i in range(len(backs)):
                if backs[i][0] == m:
                    far_first(hb * ns, lambda k: back_copy(i, k).start())
                    local_back(i)

        spectrum = functools.partial(loop, 0, each, functools.partial(transform, c))

        guard(whole, mine, work)
        if m == max(chunks - 3, 0):
            finish_planes()
        send_stage(m + 2)
        later = chunks > 2 and m == chunks - 2
        if later:
            postponed = spectrum
        elif start + count == rc:
            guard(whole, mine, spectrum)
        if m == max(chunks - 2, 0):
            cross_lines()
        done = m - 2 if chunks > 2 and m >= chunks - 1 or start else m - 1
        if chunks > 2 and m == chunks - 1:
            guard(whole, mine, postponed)
        if 0 <= done and not later and (chunks > 2 or m != chunks - 1):
            gather_back(done)
            loop(0, zl // 2, functools.partial(invert_chunk, done))

    cross_copy.wait()
    kweight = pair[zhalf] + from_pair[...]
    fetches[9].wait()
    gk = [spacing * (miller[i].reshape(rows, 128).astype(jnp.float32) + kpoint[i]) for i in range(3)]
    kdens[...] = 0.5 * (gk[0] * gk[0] + gk[1] * gk[1] + gk[2] * gk[2]) * kweight
    scaled = kweight * (-1.0 / (n * rows * 128))
    order = ((0, 0), (1, 1), (2, 2), (1, 2), (0, 2), (0, 1))
    for i, (p, q) in enumerate(order):
        part[pl.ds(i, 1), :] += fold(scaled * gk[p] * gk[q])

    group = 2 if zl % 4 == 0 else 1

    def exchange(i):
        lasts = [returned(chunks - 1, group * i + m) for m in range(group)]
        tallies = [tally[t] for t in range(len(order))]
        for j in range(2 * group):
            spot = 2 * group * i + j
            here = lasts[j // 2][:, j % 2 * width:(j % 2 + 1) * width]
            if chunks > 1:
                here = here + slopes[spot]
            g = (grad_x[spot], grad_y[spot], here)
            rise = here * here
            square[spot] = flat[spot] + rise
            weigh = above[spot] / (below[spot] + rise)
            scaled = [weigh * g[p] for p in range(3)]
            for t, (p, q) in enumerate(order):
                term = (scaled[p] * g[q]).reshape(nx // 8, 8, width)
                tallies[t] = tallies[t] + jnp.sum(term, axis=0)
        for t in range(len(order)):
            tally[t] = tallies[t]

    steps = zl // (2 * group)
    late = len(backs) - len(units)
    for i in range(chunks - 1, len(backs) - late):
        gather_back(i)
    loop(0, steps // (1 + late), exchange)
    if late:
        gather_back(len(backs) - 1)
        loop(steps // 2, steps, exchange)
    for t in range(len(order)):
        part[pl.ds(t, 1), :] += fold(tally[t])
    spots = [lax.broadcasted_iota(jnp.int32, (8, 128), i) for i in range(2)]
    sums = jnp.sum(part[...], axis=1, keepdims=True)
    row[...] = fold(jnp.where(spots[0] == spots[1], sums, 0.0))

    def stress_copy(k):
        return pltpu.make_async_remote_copy(
            row, held.at[k - 1], t_send.at[0], t_recv.at[0],
            device_id=partner(b, s, k, nb, ns), device_id_type=MESH,
        )

    def share_stress(k):
        stress_copy(k).start()

    def drain(count, semaphore):
        settle(out.at[:, pl.ds(0, count * block), :], semaphore.at[0])

    results = [
        pltpu.make_async_copy(value, target, o_sem.at[i])
        for i, (value, target) in enumerate(
            ((kdens, kdens_o), (square, square_o))
        )
    ]
    spread(n, share_stress)
    pltpu.make_async_copy(row, held.at[n - 1], t_recv.at[0]).start()
    for result in results:
        result.start()
    guard(whole, mine, functools.partial(drain, nb * na - 1, d_send))
    if not whole:
        pl.when(s >= na)(functools.partial(drain, nb * na, d_send))
    guard(whole, mine, functools.partial(drain, hb * ns - 1, g_send))
    settle(held.at[pl.ds(0, n - 1)], t_send.at[0])
    for result in results:
        result.wait()
    settle(held, t_recv.at[0])


def emit_kernel(held, kdens, square, stress_o, kdens_o, square_o, semaphores):
    step = max(square.shape[0] // 4, 1)
    pieces = [
        (square.at[pl.ds(i, step)], square_o.at[pl.ds(i, step)])
        for i in range(0, square.shape[0], step)
    ]
    pieces.append((kdens, kdens_o))
    copies = [
        pltpu.make_async_copy(source, target, semaphores.at[i])
        for i, (source, target) in enumerate(pieces)
    ]
    for copy in copies:
        copy.start()
    stress_o[...] = jnp.sum(held[...], axis=0)[0, :6]
    for copy in copies:
        copy.wait()


def params(number):
    return pltpu.CompilerParams(
        collective_id=number, has_side_effects=True, vmem_limit_bytes=60 * 2**20
    )


def vmem(*shape):
    return pltpu.VMEM(shape, jnp.float32)


def real_basis(nb, na, chunks, nx):
    xl = nx // nb
    per = xl // na
    each = per // chunks
    x = np.arange(nx)
    basis = np.zeros((chunks, nb, na, 2, each, nx))
    share = np.zeros((chunks, nb, na, 2, each))
    for b in range(nb):
        for j in range(xl):
            k = b * xl + j
            phases = (2.0 * np.pi / nx) * ((k * x) % nx)
            spot = (j % per // each, b, j // per, slice(None), j % each)
            if k % (nx // 2) == 0:
                other = (2.0 * np.pi / nx) * (((nx // 2 - k) * x) % nx)
                basis[spot] = np.stack([np.cos(phases), np.cos(other)])
                share[spot] = 1.0 / nx
            else:
                basis[spot] = np.stack([np.cos(phases), -np.sin(phases)])
                share[spot] = 2.0 / nx
    inverse = (basis * share[..., None]).reshape(chunks, 2, -1, nx)
    inverse = inverse.transpose(1, 0, 3, 2)
    return basis.reshape(chunks, -1, nx), inverse


def beside(table):
    return np.concatenate(list(host_split(table)), axis=-1)


def shards(nb, ns, coefficients, occupation, miller, density, local_factor):
    dma = pltpu.SemaphoreType.DMA
    _, zl, nx, ny = density.shape
    nzg = zl * nb
    xl = nx // nb
    na = min(ns, xl)
    per = xl // na
    chunks = min(CHUNKS, per)
    rc = 2 * (per // chunks)
    zp = zl
    while rc * zp % 8:
        zp += 1
    block = rc * zp
    npw = coefficients.shape[3]
    rows = npw // (nb * ns * 128)
    nbl = coefficients.shape[2]
    fold_y = 2 if nb % 4 == 0 else 1
    fold_z = nb // (2 * fold_y)
    hb = nb // 2

    coef = coefficients[0].reshape(2, nbl, npw // 128, 128)
    coef = coef.transpose(0, 2, 1, 3).reshape(2, npw // 128 * nbl, 128)
    basis, inverse = real_basis(nb, na, chunks, nx)
    cos_y, sin_y = fourier_tables(ny)
    cos_z, sin_z = fourier_tables(nzg)
    table_y = np.block([[cos_y, -sin_y], [sin_y, cos_y]])
    in_plane = [derivative_table(nx).astype(np.float64), derivative_table(ny).T.astype(np.float64)]
    fetched = (
        density[0],
        coef,
        local_factor,
        beside(basis),
        np.concatenate([host_split(inverse)[k] for k in (0, 0, 1)], axis=-1),
        host_split(table_y),
        host_split(derivative_table(nzg).astype(np.float64)),
        host_split(np.concatenate([cos_z, sin_z]) / (nzg * nx * ny)),
        host_split(np.stack(in_plane)),
        miller,
    )

    held, kinetic_density, square = pl.pallas_call(
        functools.partial(main_kernel, nb, ns, fold_y, fold_z),
        out_shape=(vmem(nb * ns, 1, 128), vmem(rows, 128), vmem(zl, nx, ny)),
        in_specs=[pl.BlockSpec(memory_space=pltpu.HBM)] * (len(fetched) + 1),
        out_specs=(pl.BlockSpec(memory_space=pl.ANY),) * 3,
        scratch_shapes=[pltpu.SMEM(occupation.shape, occupation.dtype)]
        + [pltpu.VMEM(value.shape, value.dtype) for value in fetched]
        + [
            pltpu.VMEM(shape, jnp.float32)
            for shape in (
                (rows, 128),
                (zl, nx, ny),
                (2, rows * nbl, 128),
                (fold_z * fold_y, 2, ns, rows, 128),
                (chunks, nb * na * block, ny),
                (chunks, ns, nb, block, ny),
                (chunks, ns, hb, block, ny),
                (chunks * hb * na * block, ny),
                (fold_z * fold_y, ns, rows, 128),
                (fold_z, fold_y, ns, rows, 128),
                (fold_y * ns - 1, fold_z, rows, 128),
                (2, fold_z // 2, rows, 128),
                (fold_z // 2 - 1, 2, rows, 128),
                (2, rows, 128),
                (rows, 128),
                (per, nzg, ny),
                (zl, nx, ny),
                (zl, nx, ny),
                (zl, nx, ny),
                (zl, nx, ny),
                (zl, nx, ny),
                (zl, nx, ny),
                (6, 8, ny),
                (8, 128),
                (1, 128),
            )
        ]
        + [dma((len(fetched) + 1,)), dma((2,))]
        + [
            dma((count,))
            for pair in (
                (1, chunks + 1), (1, 1), (fold_y * ns - 1,) * 2, (fold_z // 2 - 1,) * 2, (1, 1),
                (1, chunks + 2 if zl % 16 == 0 else chunks + 1), (1, 1),
            )
            for count in pair
        ],
        compiler_params=params(0),
        name="main_exchange",
    )(occupation, *fetched)
    anywhere = pl.BlockSpec(memory_space=pl.ANY)
    resident = pl.BlockSpec(memory_space=pltpu.VMEM)
    stress, kinetic_density, square = pl.pallas_call(
        emit_kernel,
        out_shape=[
            jax.ShapeDtypeStruct(shape, jnp.float32) for shape in ((6,), (rows, 128), (zl, nx, ny))
        ],
        in_specs=[resident, anywhere, anywhere],
        out_specs=[resident, anywhere, anywhere],
        scratch_shapes=[dma((5,))],
        compiler_params=pltpu.CompilerParams(vmem_limit_bytes=2**20),
        name="emit",
    )(held, kinetic_density, square)
    return stress, kinetic_density.reshape(rows * 128), square[None]


def solution(mesh):
    return jax.shard_map(
        functools.partial(shards, mesh.shape["band"], mesh.shape["spin"]),
        mesh=mesh,
        in_specs=(
            P("spin", None, "band", None),
            P("spin", "band"),
            P(None, ("band", "spin")),
            P("spin", "band", None, None),
            P(None, None, "band", None),
        ),
        out_specs=(P(), P(("band", "spin")), P("spin", "band", None, None)),
        check_vma=False,
    )
```
